32 devices in a mesh: dp: 8 (over y, x, core), tensor: 4 (over z).
Axes of the slice: x: 2, y: 2, z: 4, core: 2. Of those that a mesh axis runs over, the one named last changes fastest.
Arguments:
- tokens: bfloat16 [4096, 2048], P(('dp', 'tensor')), may hold values from -6 to 6
- segments: int32 [8, 512], P('dp'), may hold values from 0 to 2, never falling along the last dimension, each value on 1 to 256 neighbouring positions
- routes: int32 [4096, 6], P('dp'), may hold values from 0 to 63, all different within a row; in each aligned block of 512 rows (0 to 511, 512 to 1023, ...) at most 72 rows name the same one
- cotangent: bfloat16 [4096, 2048], P(('dp', 'tensor')), may hold values from -6 to 6
- attention_gain: bfloat16 [2048], P(('dp', 'tensor')), may hold values from 0.25 to 1.75
- latent_gain: bfloat16 [512], P(('dp', 'tensor')), may hold values from 0.25 to 1.75
- feedforward_gain: bfloat16 [2048], P(('dp', 'tensor')), may hold values from 0.25 to 1.75
- query_weight: bfloat16 [2048, 3072], P('dp', 'tensor'), may hold values from -0.125 to 0.125
- latent_weight: bfloat16 [2048, 576], P(('dp', 'tensor')), may hold values from -0.125 to 0.125
- expand_weight: bfloat16 [512, 4096], P('dp', 'tensor'), may hold values from -0.25 to 0.25
- output_weight: bfloat16 [2048, 2048], P('tensor', 'dp'), may hold values from -0.5 to 0.5
- router_weight: bfloat16 [2048, 64], P(('dp', 'tensor')), may hold values from -0.125 to 0.125
- shared_in: bfloat16 [2048, 2, 2816], P('dp', None, 'tensor'), may hold values from -0.125 to 0.125
- shared_out: bfloat16 [2816, 2048], P('tensor', 'dp'), may hold values from -0.109375 to 0.109375
- expert_in: bfloat16 [64, 2048, 2, 1408], P('dp', None, None, 'tensor'), may hold values from -0.125 to 0.125
- expert_out: bfloat16 [64, 1408, 2048], P('dp', 'tensor'), may hold values from -0.15625 to 0.15625
Outputs:
- out_tokens: bfloat16 [4096, 2048], P(('dp', 'tensor'))
- tokens_grad: float32 [4096, 2048], P(('dp', 'tensor'))
- attention_gain_grad: float32 [2048], P(('dp', 'tensor'))
- latent_gain_grad: float32 [512], P(('dp', 'tensor'))
- feedforward_gain_grad: float32 [2048], P(('dp', 'tensor'))
- query_weight_grad: float32 [2048, 3072], P('dp', 'tensor')
- latent_weight_grad: float32 [2048, 576], P(('dp', 'tensor'))
- expand_weight_grad: float32 [512, 4096], P('dp', 'tensor')
- output_weight_grad: float32 [2048, 2048], P('tensor', 'dp')
- router_weight_grad: float32 [2048, 64], P(('dp', 'tensor'))
- shared_in_grad: float32 [2048, 2, 2816], P('dp', None, 'tensor')
- shared_out_grad: float32 [2816, 2048], P('tensor', 'dp')
- expert_in_grad: float32 [64, 2048, 2, 1408], P('dp', None, None, 'tensor')
- expert_out_grad: float32 [64, 1408, 2048], P('dp', 'tensor')
The draws below stay inside these ranges and needn't reach their ends.
Inputs may be any that keep to these rules, and one draw needn't show every extreme that they name: `segments`: each row numbers the sequences of one group in order; a sequence holds at most 256 tokens and one holds exactly that many. `routes`: the 6 experts of a token differ. Within the 512 tokens of one index of dp, no expert is named more than 72 times, a bound that some block reaches.
All inputs are finite; a program needn't handle non-finite values.
Results may differ from the reference program's by a relative error of at most 0.024.
Values may be sent and summed in bfloat16 or wider, within the bound.
A program may use at most 512 MiB of HBM per device.

```python
import math
import jax
import jax.numpy as jnp
import numpy as np
from jax import lax

D = 2048
H = 16
DN = 128
DR = 64
DV = 128
KVR = 512
EXPERTS = 64
FFE = 1408
FFS = 2816
TOPK = 6
GROUP = 512
SEQS = 3
SEQ_MAX = 256
CAP = 72
TOKENS = 4096
N_DP = 8
N_TENSOR = 4


def block_scale(key, extent, split, low, largest):
    level, own = 1.0, jax.random.fold_in(key, 6)
    for axis_at, shards_of in split:
        heights = jnp.exp(jax.random.uniform(jax.random.fold_in(own, axis_at), (shards_of,), jnp.float32, low / len(split), largest / len(split)))
        level = level * jnp.repeat(heights, extent[axis_at] // shards_of).reshape([-1 if axis == axis_at else 1 for axis in range(len(extent))])
    return level


def profile(count, total, most, lean):
    weights = [(1 << 20) // math.isqrt(rank ** lean) + 1 for rank in range(2, count + 1)]
    surplus, holding = total - most - (count - 1), [1] * (count - 1)
    while surplus > 0:
        free = [i for i in range(count - 1) if holding[i] < most]
        mass, left = sum([weights[i] for i in free]), surplus
        for i in free:
            more = min(most - holding[i], max(1, left * weights[i] // mass), surplus)
            holding[i] = holding[i] + more
            surplus = surplus - more
    return np.array([most] + holding)


def ragged_sizes(rng, amount, total, limit, skew):
    if amount == 2:
        one = jax.random.randint(rng, (), max(1, total - limit), min(limit, total - 1) + 1)
        return jnp.stack([one, total - one])
    lengths = jnp.asarray(profile(amount, total, limit, skew), jnp.int32)
    twos = (amount - 1) // 2
    donor, taker = lengths[1:1 + 2 * twos:2], lengths[2:2 + 2 * twos:2]
    slack = jnp.minimum(donor - 1, limit - taker)
    passed = jax.random.randint(jax.random.fold_in(rng, 1), (twos,), 0, 1 << 20) % (slack + 1)
    lengths = lengths.at[1:1 + 2 * twos:2].set(donor - passed).at[2:2 + 2 * twos:2].set(taker + passed)
    return lengths[jax.random.permutation(jax.random.fold_in(rng, 2), amount)]


def assign_block(key, own, number, rows, count, top, most, skew):
    order = jax.random.permutation(key, count)
    heavy_load, ordinary = portions_of(count, rows * top, most, skew, True), portions_of(count, rows * top, most, skew, False)
    places = jnp.arange(count)

    def named(lengths, turn):
        used = int((lengths > 0).sum())
        fixed = max(1, used // 4)
        shifted = fixed + (places - fixed + turn * (used - fixed)) % max(1, count - fixed)
        return jnp.zeros((count,), jnp.int32).at[order[jnp.where(places < fixed, places, shifted)]].set(jnp.asarray(lengths, jnp.int32))

    lengths = jnp.where(number % 4 == 0, named(heavy_load, number // 4), named(ordinary, number - number // 4 - 1))
    mixed = jax.random.permutation(jax.random.fold_in(own, 3), count)
    donor, receiver = mixed[0:count // 2 * 2:2], mixed[1:count // 2 * 2:2]
    margin = jnp.minimum(lengths[donor] - 1, most - lengths[receiver]) // 2
    margin = jnp.where((donor == order[0]) | (receiver == order[0]) | (lengths[receiver] == 0), 0, jnp.maximum(margin, 0))
    shifted = jax.random.randint(jax.random.fold_in(own, 4), (count // 2,), 0, 1 << 20) % (margin + 1)
    lengths = lengths.at[donor].add(-shifted).at[receiver].add(shifted)
    labels = jnp.searchsorted(jnp.cumsum(lengths), jnp.arange(rows * top), side="right").astype(jnp.int32)
    grid = labels.reshape(top, rows).T
    grid = grid[jax.random.permutation(jax.random.fold_in(own, 1), rows)]
    turn = jax.random.randint(jax.random.fold_in(own, 2), (rows, 1), 0, top)
    return jnp.take_along_axis(grid, (jnp.arange(top)[None, :] + turn) % top, axis=1)


def portions_of(count, total, limit, slope, full):
    weights = [(1 << 20) // math.isqrt(standing ** slope) + 1 for standing in range(1, count + 1)]
    largest = limit if full else min(limit, max(-(-total // count), total * weights[0] // sum(weights)))
    least = 1 if total - largest >= count - 1 else 0
    counts, rest = [largest] + [least] * (count - 1), total - largest - least * (count - 1)
    while rest > 0:
        movable = [i for i in range(1, count) if counts[i] < largest] or [i for i in range(1, count) if counts[i] < limit]
        pool, budget = sum([weights[i] for i in movable]), rest
        for i in movable:
            extra = min(limit - counts[i], max(1, budget * weights[i] // pool), rest)
            counts[i] = counts[i] + extra
            rest = rest - extra
    return np.array(counts)


def gaussian(own_key, shape, scale, bound, cuts=(), kind=jnp.bfloat16):
    values = scale * jax.random.normal(own_key, shape, jnp.float32)
    if cuts:
        values = values * block_scale(own_key, shape, cuts, -0.22, 0.18)
    return jnp.clip(values, -bound, bound).astype(kind)


def setup_inputs(seed: int = 0) -> dict:
    seeds = jax.random.split(jax.random.key(seed), 17)
    tokens = gaussian(seeds[0], (TOKENS, D), 1.0, 6.0, ((0, 32),))
    segments = jax.vmap(lambda own: jnp.searchsorted(jnp.cumsum(ragged_sizes(own, SEQS, GROUP, SEQ_MAX, 2)), jnp.arange(GROUP), side="right"))(jax.random.split(seeds[1], N_DP)).reshape((N_DP, GROUP)).astype(jnp.int32)
    routes_keys = jax.random.split(jax.random.fold_in(seeds[2], 1), TOKENS // GROUP)
    routes_turns = jax.random.permutation(jax.random.fold_in(seeds[2], 3), TOKENS // GROUP)
    routes = jax.vmap(lambda own, number: assign_block(jax.random.fold_in(seeds[2], 2), own, number, GROUP, EXPERTS, TOPK, CAP, 2))(routes_keys, routes_turns).reshape((TOKENS, TOPK))
    cotangent = gaussian(seeds[3], (TOKENS, D), 1.0, 6.0, ((0, 32),))
    attention_gain = jnp.clip(1.0 + 0.15 * jax.random.normal(seeds[4], (D,), jnp.float32), 0.25, 1.75).astype(jnp.bfloat16)
    latent_gain = jnp.clip(1.0 + 0.15 * jax.random.normal(seeds[5], (KVR,), jnp.float32), 0.25, 1.75).astype(jnp.bfloat16)
    feedforward_gain = jnp.clip(1.0 + 0.15 * jax.random.normal(seeds[6], (D,), jnp.float32), 0.25, 1.75).astype(jnp.bfloat16)
    query_weight = gaussian(seeds[7], (D, H * (DN + DR)), D ** -0.5, 0.125, ((0, 8), (1, 4)))
    latent_weight = gaussian(seeds[8], (D, KVR + DR), D ** -0.5, 0.125, ((0, 32),))
    expand_weight = gaussian(seeds[9], (KVR, H * (DN + DV)), KVR ** -0.5, 0.25, ((0, 8), (1, 4)))
    output_weight = gaussian(seeds[10], (H * DV, D), (H * DV // 16) ** -0.5, 0.5, ((0, 4), (1, 8)))
    router_weight = gaussian(seeds[11], (D, EXPERTS), D ** -0.5, 0.125, ((0, 32),))
    shared_in = gaussian(seeds[12], (D, 2, FFS), D ** -0.5, 0.125, ((0, 8), (2, 4)))
    shared_out = gaussian(seeds[13], (FFS, D), FFS ** -0.5, 0.109375, ((0, 4), (1, 8)))
    expert_in = gaussian(seeds[14], (EXPERTS, D, 2, FFE), D ** -0.5, 0.125, ((0, 8), (3, 4)))
    expert_out = gaussian(seeds[15], (EXPERTS, FFE, D), FFE ** -0.5, 0.15625, ((0, 8), (1, 4)))
    return {"tokens": tokens, "segments": segments, "routes": routes, "cotangent": cotangent, "attention_gain": attention_gain, "latent_gain": latent_gain, "feedforward_gain": feedforward_gain, "query_weight": query_weight, "latent_weight": latent_weight, "expand_weight": expand_weight, "output_weight": output_weight, "router_weight": router_weight, "shared_in": shared_in, "shared_out": shared_out, "expert_in": expert_in, "expert_out": expert_out}


epsilon = 1e-06
route_scale = 2.446
rope_base = 50000.0
excluded = -1e+30

def rms_scale(array_in):
    return lax.rsqrt(lax.optimization_barrier(jnp.mean(array_in * array_in, axis=-1, keepdims=True)) + epsilon)

def rope_tables(segment_row):
    places = jnp.arange(segment_row.shape[0], dtype=jnp.int32)
    boundary = jnp.concatenate([jnp.ones((1,), jnp.bool_), segment_row[1:] != segment_row[:-1]])
    begins = lax.cummax(jnp.where(boundary, places, 0), axis=0)
    position = (places - begins).astype(jnp.float32)
    freqs = rope_base ** (-jnp.arange(DR // 2, dtype=jnp.float32) * 2.0 / DR)
    angle = position[:, None] * freqs[None, :]
    return (jnp.cos(angle), jnp.sin(angle))

def rotate(array_in, cosine, sine):
    half_width = array_in.shape[-1] // 2
    first_half, second_half = (array_in[..., :half_width], array_in[..., half_width:])
    return jnp.concatenate([first_half * cosine - second_half * sine, second_half * cosine + first_half * sine], axis=-1)

def unrotate(array_in, cosine, sine):
    half_width = array_in.shape[-1] // 2
    first_half, second_half = (array_in[..., :half_width], array_in[..., half_width:])
    return jnp.concatenate([first_half * cosine + second_half * sine, second_half * cosine - first_half * sine], axis=-1)

def attention_tables(normed, query_weight, latent_weight, expand_weight, latent_gain, cosine, sine):
    row_count = normed.shape[0]
    head_count = query_weight.shape[1] // (DN + DR)
    query = jnp.dot(normed, query_weight, preferred_element_type=jnp.float32).reshape(row_count, head_count, DN + DR)
    query = jnp.concatenate([query[..., :DN], rotate(query[..., DN:], cosine[:, None, :], sine[:, None, :])], axis=-1).astype(jnp.bfloat16)
    latent = jnp.dot(normed, latent_weight, preferred_element_type=jnp.float32)
    compressed = latent[:, :KVR]
    latent_scale = rms_scale(compressed)
    latent_normed = (compressed * latent_scale * latent_gain.astype(jnp.float32)).astype(jnp.bfloat16)
    rope_key = rotate(latent[:, KVR:], cosine, sine)
    keyvalue = jnp.dot(latent_normed, expand_weight, preferred_element_type=jnp.float32).reshape(row_count, head_count, DN + DV)
    key_rows = jnp.concatenate([keyvalue[..., :DN], jnp.broadcast_to(rope_key[:, None, :], (row_count, head_count, DR))], axis=-1).astype(jnp.bfloat16)
    value_rows = keyvalue[..., DN:].astype(jnp.bfloat16)
    return (query, key_rows, value_rows, compressed, latent_scale, latent_normed)

def masked_scores(query_block, key_rows, start, segment_row):
    block_rows = query_block.shape[0]
    head_depth = query_block.shape[-1]
    scores = jnp.einsum('qhd,khd->hqk', query_block.astype(jnp.float32), key_rows.astype(jnp.float32)) * head_depth ** (-0.5)
    row_index = start + jnp.arange(block_rows, dtype=jnp.int32)
    column_index = jnp.arange(key_rows.shape[0], dtype=jnp.int32)
    row_segments = lax.dynamic_slice_in_dim(segment_row, start, block_rows)
    allowed = (segment_row[None, :] == row_segments[:, None]) & (column_index[None, :] <= row_index[:, None])
    return jnp.where(allowed[None], scores, excluded)

def attend(query, key_rows, value_rows, segment_row):
    row_count, head_count, head_depth = query.shape
    block_rows = min(row_count, 512)
    blocks = row_count // block_rows
    starts = jnp.arange(blocks, dtype=jnp.int32) * block_rows

    def one_block(inputs):
        query_block, start = inputs
        scores = masked_scores(query_block, key_rows, start, segment_row)
        logsum = jnp.log(lax.optimization_barrier(jnp.sum(jnp.exp(scores), axis=-1)))
        weights_low = jnp.exp(scores - logsum[..., None]).astype(jnp.bfloat16)
        mixed = jnp.einsum('hqk,khd->qhd', weights_low.astype(jnp.float32), value_rows.astype(jnp.float32)).astype(jnp.bfloat16)
        return (mixed, logsum.T)
    mixed, logsum = lax.map(one_block, (query.reshape(blocks, block_rows, head_count, head_depth), starts))
    return (mixed.reshape(row_count, head_count, -1), logsum.reshape(row_count, head_count))

def attend_back(query, key_rows, value_rows, segment_row, out_grad, logsum):
    row_count, head_count, head_depth = query.shape
    block_rows = min(row_count, 512)
    blocks = row_count // block_rows
    starts = jnp.arange(blocks, dtype=jnp.int32) * block_rows

    def one_block(carry, inputs):
        key_grad, value_grad = carry
        query_block, grad_block, logsum_block, start = inputs
        scores = masked_scores(query_block, key_rows, start, segment_row)
        weights_full = jnp.exp(scores - logsum_block.T[..., None])
        weights_low = weights_full.astype(jnp.bfloat16)
        prob_grad = jnp.einsum('qhd,khd->hqk', grad_block.astype(jnp.float32), value_rows.astype(jnp.float32))
        row_total = lax.optimization_barrier(jnp.sum(weights_full * prob_grad, axis=-1, keepdims=True))
        score_grad = (weights_full * (prob_grad - row_total) * head_depth ** (-0.5)).astype(jnp.bfloat16)
        query_grad = jnp.einsum('hqk,khd->qhd', score_grad.astype(jnp.float32), key_rows.astype(jnp.float32))
        key_grad = key_grad + jnp.einsum('hqk,qhd->khd', score_grad.astype(jnp.float32), query_block.astype(jnp.float32))
        value_grad = value_grad + jnp.einsum('hqk,qhd->khd', weights_low.astype(jnp.float32), grad_block.astype(jnp.float32))
        return ((key_grad, value_grad), query_grad)
    initial = (jnp.zeros((row_count, head_count, head_depth), jnp.float32), jnp.zeros((row_count, head_count, value_rows.shape[-1]), jnp.float32))
    (key_grad, value_grad), query_grad = lax.scan(one_block, initial, (query.reshape(blocks, block_rows, head_count, head_depth), out_grad.reshape(blocks, block_rows, head_count, -1), logsum.reshape(blocks, block_rows, head_count), starts))
    return (query_grad.reshape(row_count, head_count, head_depth), key_grad, value_grad)

def expert_slots(route_group):
    route_flat = route_group.reshape(-1)
    onehot = (route_flat[:, None] == jnp.arange(EXPERTS, dtype=jnp.int32)[None, :]).astype(jnp.int32)
    before = jnp.cumsum(onehot, axis=0) - onehot
    return (route_flat, lax.optimization_barrier(jnp.sum(before * onehot, axis=1)).astype(jnp.int32))

def expert_forward_one(rows_in, weight_in, weight_out):
    row_count = rows_in.shape[0]
    pre = jnp.dot(rows_in, weight_in.reshape(D, 2 * FFE), preferred_element_type=jnp.float32).reshape(row_count, 2, FFE)
    activation = (jax.nn.silu(pre[:, 0]) * pre[:, 1]).astype(jnp.bfloat16)
    quarter = FFE // N_TENSOR
    total = jnp.zeros((row_count, D), jnp.float32)
    for part in range(N_TENSOR):
        piece = jnp.dot(activation[:, part * quarter:(part + 1) * quarter], weight_out[part * quarter:(part + 1) * quarter], preferred_element_type=jnp.float32)
        total = total + lax.optimization_barrier(piece.astype(jnp.bfloat16)).astype(jnp.float32)
    return total

def expert_backward_one(rows_in, grads_in, weight_in, weight_out):
    row_count = rows_in.shape[0]
    pre = jnp.dot(rows_in, weight_in.reshape(D, 2 * FFE), preferred_element_type=jnp.float32).reshape(row_count, 2, FFE)
    gate_pre, up_pre = (pre[:, 0], pre[:, 1])
    sigm = jax.nn.sigmoid(gate_pre)
    activation = jax.nn.silu(gate_pre)
    hidden_act = (activation * up_pre).astype(jnp.bfloat16)
    hidden_grad = jnp.dot(grads_in, weight_out.T, preferred_element_type=jnp.float32)
    pre_grad = jnp.stack([hidden_grad * up_pre * sigm * (1.0 + gate_pre * (1.0 - sigm)), hidden_grad * activation], axis=1).astype(jnp.bfloat16)
    out_weight_grad = jnp.dot(hidden_act.T, grads_in, preferred_element_type=jnp.float32)
    in_weight_grad = jnp.dot(rows_in.T, pre_grad.reshape(row_count, 2 * FFE), preferred_element_type=jnp.float32).reshape(D, 2, FFE)
    quarter = FFE // N_TENSOR
    row_grad = jnp.zeros((row_count, D), jnp.float32)
    for part in range(N_TENSOR):
        lows = pre_grad[:, :, part * quarter:(part + 1) * quarter].reshape(row_count, 2 * quarter)
        weights_part = weight_in[:, :, part * quarter:(part + 1) * quarter].reshape(D, 2 * quarter)
        piece = jnp.dot(lows, weights_part.T, preferred_element_type=jnp.float32)
        row_grad = row_grad + lax.optimization_barrier(piece.astype(jnp.bfloat16)).astype(jnp.float32)
    return (in_weight_grad, out_weight_grad, row_grad)

def reference(tokens, segments, routes, cotangent, attention_gain, latent_gain, feedforward_gain, query_weight, latent_weight, expand_weight, output_weight, router_weight, shared_in, shared_out, expert_in, expert_out):
    token_groups = tokens.reshape(N_DP, GROUP, D)
    grad_groups = cotangent.reshape(N_DP, GROUP, D)
    route_groups = routes.reshape(N_DP, GROUP, TOPK)
    places = jnp.arange(N_DP, dtype=jnp.int32)
    gain_one = attention_gain.astype(jnp.float32)
    gain_two = feedforward_gain.astype(jnp.float32)

    def front(inputs):
        group_rows, segment_row, route_group = inputs
        wide = group_rows.astype(jnp.float32)
        normed = (wide * rms_scale(wide) * gain_one).astype(jnp.bfloat16)
        cosine, sine = rope_tables(segment_row)
        query, key_rows, value_rows, _, _, _ = attention_tables(normed, query_weight, latent_weight, expand_weight, latent_gain, cosine, sine)
        mixed, _ = attend(query, key_rows, value_rows, segment_row)
        hidden = wide + jnp.dot(mixed.reshape(GROUP, H * DV), output_weight, preferred_element_type=jnp.float32)
        normed_two = (hidden * rms_scale(hidden) * gain_two).astype(jnp.bfloat16)
        route_flat, slot_index = expert_slots(route_group)
        buffer = jnp.zeros((EXPERTS, CAP, D), jnp.bfloat16).at[route_flat, slot_index].set(jnp.repeat(normed_two, TOPK, axis=0))
        return (hidden, buffer)
    hiddens, buffers = lax.map(front, (token_groups, segments, route_groups))

    def expert_fwd(inputs):
        index, weight_in, weight_out = inputs
        rows_in = buffers[:, index].reshape(N_DP * CAP, D)
        return expert_forward_one(rows_in, weight_in, weight_out)
    expert_outs = lax.map(expert_fwd, (jnp.arange(EXPERTS, dtype=jnp.int32), expert_in, expert_out))

    def middle(carry, inputs):
        shared_in_acc, shared_out_acc, router_acc = carry
        hidden, grad_rows, route_group, place = inputs
        normed_two = (hidden * rms_scale(hidden) * gain_two).astype(jnp.bfloat16)
        logits = jnp.dot(normed_two, router_weight, preferred_element_type=jnp.float32)
        sigm = jax.nn.sigmoid(logits)
        chosen = route_group[:, :, None] == jnp.arange(EXPERTS, dtype=jnp.int32)[None, None, :]
        picked = lax.optimization_barrier(jnp.sum(jnp.where(chosen, sigm[:, None, :], 0.0), axis=-1))
        picked_total = lax.optimization_barrier(jnp.sum(picked, axis=1, keepdims=True))
        gate_weights = route_scale * picked / picked_total
        pre = jnp.dot(normed_two, shared_in.reshape(D, 2 * FFS), preferred_element_type=jnp.float32).reshape(GROUP, 2, FFS)
        shared_act = (jax.nn.silu(pre[:, 0]) * pre[:, 1]).astype(jnp.bfloat16)
        shared_part = jnp.dot(shared_act, shared_out, preferred_element_type=jnp.float32)
        route_flat, slot_index = expert_slots(route_group)
        routed = expert_outs[route_flat, place * CAP + slot_index].reshape(GROUP, TOPK, D)
        out_group = (hidden + shared_part + lax.optimization_barrier(jnp.sum(gate_weights[..., None] * routed, axis=1))).astype(jnp.bfloat16)
        grad_wide = grad_rows.astype(jnp.float32)
        gate_grad = lax.optimization_barrier(jnp.sum(routed * grad_wide[:, None, :], axis=-1))
        routed_grad = (gate_weights[..., None] * grad_wide[:, None, :]).astype(jnp.bfloat16)
        grad_buffer = jnp.zeros((EXPERTS, CAP, D), jnp.bfloat16).at[route_flat, slot_index].set(routed_grad.reshape(GROUP * TOPK, D))
        sig_shared = jax.nn.sigmoid(pre[:, 0])
        hid_grad = jnp.dot(grad_rows, shared_out.T, preferred_element_type=jnp.float32)
        pre_grad = jnp.stack([hid_grad * pre[:, 1] * sig_shared * (1.0 + pre[:, 0] * (1.0 - sig_shared)), hid_grad * jax.nn.silu(pre[:, 0])], axis=1).astype(jnp.bfloat16)
        shared_out_acc = shared_out_acc + jnp.dot(shared_act.T, grad_rows, preferred_element_type=jnp.float32)
        shared_in_acc = shared_in_acc + jnp.dot(normed_two.T, pre_grad.reshape(GROUP, 2 * FFS), preferred_element_type=jnp.float32).reshape(D, 2, FFS)
        input_grad = jnp.dot(pre_grad.reshape(GROUP, 2 * FFS), shared_in.reshape(D, 2 * FFS).T, preferred_element_type=jnp.float32)
        picked_grad = route_scale * (gate_grad / picked_total - lax.optimization_barrier(jnp.sum(gate_grad * picked, axis=1, keepdims=True)) / (picked_total * picked_total))
        logit_part = picked_grad * picked * (1.0 - picked)
        logit_grad = lax.optimization_barrier(jnp.sum(jnp.where(chosen, logit_part[..., None], 0.0), axis=1))
        router_acc = router_acc + jnp.dot(normed_two.astype(jnp.float32).T, logit_grad, precision=lax.Precision.HIGHEST)
        input_grad = input_grad + jnp.dot(logit_grad, router_weight.astype(jnp.float32).T, precision=lax.Precision.HIGHEST)
        return ((shared_in_acc, shared_out_acc, router_acc), (out_group, grad_buffer, input_grad))
    start_mid = (jnp.zeros((D, 2, FFS), jnp.float32), jnp.zeros((FFS, D), jnp.float32), jnp.zeros((D, EXPERTS), jnp.float32))
    (shared_in_grad, shared_out_grad, router_weight_grad), (out_groups, grad_buffers, input_grads) = lax.scan(middle, start_mid, (hiddens, grad_groups, route_groups, places))

    def expert_bwd(inputs):
        index, weight_in, weight_out = inputs
        rows_in = buffers[:, index].reshape(N_DP * CAP, D)
        grads_in = grad_buffers[:, index].reshape(N_DP * CAP, D)
        return expert_backward_one(rows_in, grads_in, weight_in, weight_out)
    expert_in_grad, expert_out_grad, row_grads = lax.map(expert_bwd, (jnp.arange(EXPERTS, dtype=jnp.int32), expert_in, expert_out))

    def back(carry, inputs):
        gain_one_acc, gain_lat_acc, gain_two_acc, query_acc, latent_acc, expand_acc, output_acc = carry
        group_rows, hidden, grad_rows, segment_row, route_group, place, input_grad = inputs
        route_flat, slot_index = expert_slots(route_group)
        routed_back = lax.optimization_barrier(jnp.sum(row_grads[route_flat, place * CAP + slot_index].reshape(GROUP, TOPK, D), axis=1))
        normed_two_grad = input_grad + routed_back
        scale_two = rms_scale(hidden)
        weighted = normed_two_grad * gain_two
        gain_two_acc = gain_two_acc + lax.optimization_barrier(jnp.sum(normed_two_grad * hidden * scale_two, axis=0))
        hidden_grad = grad_rows.astype(jnp.float32) + scale_two * weighted - hidden * scale_two ** 3 * lax.optimization_barrier(jnp.mean(hidden * weighted, axis=-1, keepdims=True))
        wide = group_rows.astype(jnp.float32)
        scale_one = rms_scale(wide)
        normed = (wide * scale_one * gain_one).astype(jnp.bfloat16)
        cosine, sine = rope_tables(segment_row)
        query, key_rows, value_rows, compressed, latent_scale, latent_normed = attention_tables(normed, query_weight, latent_weight, expand_weight, latent_gain, cosine, sine)
        mixed, logsum = attend(query, key_rows, value_rows, segment_row)
        hidden_low = hidden_grad.astype(jnp.bfloat16)
        output_acc = output_acc + jnp.dot(mixed.reshape(GROUP, H * DV).T, hidden_low, preferred_element_type=jnp.float32)
        mixed_grad = jnp.dot(hidden_low, output_weight.T, preferred_element_type=jnp.float32).astype(jnp.bfloat16).reshape(GROUP, H, DV)
        query_grad, key_grad, value_grad = attend_back(query, key_rows, value_rows, segment_row, mixed_grad, logsum)
        query_pre = jnp.concatenate([query_grad[..., :DN], unrotate(query_grad[..., DN:], cosine[:, None, :], sine[:, None, :])], axis=-1).astype(jnp.bfloat16).reshape(GROUP, H * (DN + DR))
        query_acc = query_acc + jnp.dot(normed.T, query_pre, preferred_element_type=jnp.float32)
        normed_grad = jnp.dot(query_pre, query_weight.T, preferred_element_type=jnp.float32)
        keyvalue_grad = jnp.concatenate([key_grad[..., :DN], value_grad], axis=-1).astype(jnp.bfloat16).reshape(GROUP, H * (DN + DV))
        expand_acc = expand_acc + jnp.dot(latent_normed.T, keyvalue_grad, preferred_element_type=jnp.float32)
        latent_normed_grad = jnp.dot(keyvalue_grad, expand_weight.T, preferred_element_type=jnp.float32)
        rope_grad = unrotate(lax.optimization_barrier(jnp.sum(key_grad[..., DN:], axis=1)), cosine, sine)
        lat_weighted = latent_normed_grad * latent_gain.astype(jnp.float32)
        gain_lat_acc = gain_lat_acc + lax.optimization_barrier(jnp.sum(latent_normed_grad * compressed * latent_scale, axis=0))
        compressed_grad = latent_scale * lat_weighted - compressed * latent_scale ** 3 * lax.optimization_barrier(jnp.mean(compressed * lat_weighted, axis=-1, keepdims=True))
        latent_grad = jnp.concatenate([compressed_grad, rope_grad], axis=-1)
        latent_acc = latent_acc + jnp.dot(normed.astype(jnp.float32).T, latent_grad, precision=lax.Precision.HIGHEST)
        normed_grad = normed_grad + jnp.dot(latent_grad, latent_weight.astype(jnp.float32).T, precision=lax.Precision.HIGHEST)
        weighted_one = normed_grad * gain_one
        gain_one_acc = gain_one_acc + lax.optimization_barrier(jnp.sum(normed_grad * wide * scale_one, axis=0))
        token_grad = hidden_grad + scale_one * weighted_one - wide * scale_one ** 3 * lax.optimization_barrier(jnp.mean(wide * weighted_one, axis=-1, keepdims=True))
        return ((gain_one_acc, gain_lat_acc, gain_two_acc, query_acc, latent_acc, expand_acc, output_acc), token_grad)
    start_back = (jnp.zeros((D,), jnp.float32), jnp.zeros((KVR,), jnp.float32), jnp.zeros((D,), jnp.float32), jnp.zeros((D, H * (DN + DR)), jnp.float32), jnp.zeros((D, KVR + DR), jnp.float32), jnp.zeros((KVR, H * (DN + DV)), jnp.float32), jnp.zeros((H * DV, D), jnp.float32))
    grads_back, token_grads = lax.scan(back, start_back, (token_groups, hiddens, grad_groups, segments, route_groups, places, input_grads))
    gain_one_grad, gain_lat_grad, gain_two_grad, query_weight_grad, latent_weight_grad, expand_weight_grad, output_weight_grad = grads_back
    return (out_groups.reshape(TOKENS, D), token_grads.reshape(TOKENS, D), gain_one_grad, gain_lat_grad, gain_two_grad, query_weight_grad, latent_weight_grad, expand_weight_grad, output_weight_grad, router_weight_grad, shared_in_grad, shared_out_grad, expert_in_grad, expert_out_grad)
```

```python
import jax
import jax.numpy as jnp
from jax import lax
from jax.sharding import PartitionSpec as P

DN = 128
DR = 64
DV = 128
KVR = 512
EXPERTS = 64
TOPK = 6
CAP = 72
BOTH = ("dp", "tensor")


epsilon = 1e-06
route_scale = 2.446
rope_base = 50000.0
excluded = -1e30


def rms_scale(array_in):
    return lax.rsqrt(jnp.mean(array_in * array_in, axis=-1, keepdims=True) + epsilon)


def rope_tables(segment_row):
    places = jnp.arange(segment_row.shape[0], dtype=jnp.int32)
    begins = jnp.sum((segment_row[None, :] < segment_row[:, None]).astype(jnp.int32), axis=1)
    position = (places - begins).astype(jnp.float32)
    freqs = rope_base ** (-jnp.arange(DR // 2, dtype=jnp.float32) * 2.0 / DR)
    angle = position[:, None] * freqs[None, :]
    return (jnp.cos(angle), jnp.sin(angle))


def rotate(array_in, cosine, sine):
    half_width = array_in.shape[-1] // 2
    first_half, second_half = (array_in[..., :half_width], array_in[..., half_width:])
    return jnp.concatenate(
        [first_half * cosine - second_half * sine, second_half * cosine + first_half * sine],
        axis=-1,
    )


def unrotate(array_in, cosine, sine):
    half_width = array_in.shape[-1] // 2
    first_half, second_half = (array_in[..., :half_width], array_in[..., half_width:])
    return jnp.concatenate(
        [first_half * cosine + second_half * sine, second_half * cosine - first_half * sine],
        axis=-1,
    )


def attention_tables(normed, query_weight, latent_weight, expand_weight, latent_gain, cosine, sine):
    row_count = normed.shape[0]
    head_count = query_weight.shape[1] // (DN + DR)
    query = jnp.dot(normed, query_weight, preferred_element_type=jnp.float32).reshape(
        row_count, head_count, DN + DR
    )
    query = jnp.concatenate(
        [query[..., :DN], rotate(query[..., DN:], cosine[:, None, :], sine[:, None, :])], axis=-1
    ).astype(jnp.bfloat16)
    latent = jnp.dot(normed, latent_weight, preferred_element_type=jnp.float32)
    compressed = latent[:, :KVR]
    latent_scale = rms_scale(compressed)
    latent_normed = (compressed * latent_scale * latent_gain.astype(jnp.float32)).astype(
        jnp.bfloat16
    )
    rope_key = rotate(latent[:, KVR:], cosine, sine)
    keyvalue = jnp.dot(latent_normed, expand_weight, preferred_element_type=jnp.float32).reshape(
        row_count, head_count, DN + DV
    )
    key_rows = jnp.concatenate(
        [keyvalue[..., :DN], jnp.broadcast_to(rope_key[:, None, :], (row_count, head_count, DR))],
        axis=-1,
    ).astype(jnp.bfloat16)
    value_rows = keyvalue[..., DN:].astype(jnp.bfloat16)
    return (query, key_rows, value_rows, compressed, latent_scale, latent_normed)


def masked_scores(query, key_rows, segment_row):
    scores = jnp.einsum(
        "qhd,khd->hqk", query, key_rows, preferred_element_type=jnp.float32
    ) * query.shape[-1] ** (-0.5)
    places = jnp.arange(key_rows.shape[0], dtype=jnp.int32)
    allowed = (segment_row[None, :] == segment_row[:, None]) & (places[None, :] <= places[:, None])
    return jnp.where(allowed[None], scores, excluded)


def attend(query, key_rows, value_rows, segment_row):
    scores = masked_scores(query, key_rows, segment_row)
    logsum = jnp.log(jnp.sum(jnp.exp(scores), axis=-1))
    weights_low = jnp.exp(scores - logsum[..., None]).astype(jnp.bfloat16)
    mixed = jnp.einsum(
        "hqk,khd->qhd", weights_low, value_rows, preferred_element_type=jnp.float32
    ).astype(jnp.bfloat16)
    return (mixed, logsum)


def attend_back(query, key_rows, value_rows, segment_row, out_grad, logsum):
    scores = masked_scores(query, key_rows, segment_row)
    weights_full = jnp.exp(scores - logsum[..., None])
    weights_low = weights_full.astype(jnp.bfloat16)
    prob_grad = jnp.einsum("qhd,khd->hqk", out_grad, value_rows, preferred_element_type=jnp.float32)
    row_total = jnp.sum(weights_full * prob_grad, axis=-1, keepdims=True)
    score_grad = (weights_full * (prob_grad - row_total) * query.shape[-1] ** (-0.5)).astype(
        jnp.bfloat16
    )
    query_grad = jnp.einsum("hqk,khd->qhd", score_grad, key_rows, preferred_element_type=jnp.float32)
    key_grad = jnp.einsum("hqk,qhd->khd", score_grad, query, preferred_element_type=jnp.float32)
    value_grad = jnp.einsum("hqk,qhd->khd", weights_low, out_grad, preferred_element_type=jnp.float32)
    return (query_grad, key_grad, value_grad)


def swiglu_grad(hidden_grad, gate_pre, up_pre):
    sigm = jax.nn.sigmoid(gate_pre)
    return (
        hidden_grad * up_pre * sigm * (1.0 + gate_pre * (1.0 - sigm)),
        hidden_grad * jax.nn.silu(gate_pre),
    )


def gather(array_in, axis_name, axis=0):
    return lax.all_gather(array_in, axis_name, axis=axis, tiled=True)


def scatter_sum(array_in, axis_name, axis=0):
    return lax.psum_scatter(array_in, axis_name, scatter_dimension=axis, tiled=True)


def own_slice(array_in, first_row, own_rows):
    return lax.dynamic_slice_in_dim(array_in, first_row, own_rows, 0)


def body(
    tokens,
    segments,
    routes,
    cotangent,
    attention_gain,
    latent_gain,
    feedforward_gain,
    query_weight,
    latent_weight,
    expand_weight,
    output_weight,
    router_weight,
    shared_in,
    shared_out,
    expert_in,
    expert_out,
):
    own_rows, width = tokens.shape
    groups = lax.axis_size("dp")
    place_dp = lax.axis_index("dp")
    first_row = lax.axis_index("tensor") * own_rows
    local_experts = expert_in.shape[0]
    segment_row = segments[0]
    group_rows = gather(tokens, "tensor")
    row_count = group_rows.shape[0]
    gain_one_low, gain_lat_low, gain_two_low = (
        gather(attention_gain, BOTH),
        gather(latent_gain, BOTH),
        gather(feedforward_gain, BOTH),
    )
    latent_full = gather(latent_weight, BOTH)
    expand_full = gather(expand_weight, "dp")
    query_full = gather(query_weight, "dp")
    output_full = gather(output_weight, "dp", 1)
    router_full = gather(router_weight, BOTH)
    routes_all = gather(routes, "dp")
    shared_in_full = gather(shared_in, "dp")
    shared_out_full = gather(shared_out, "dp", 1)
    gain_one = gain_one_low.astype(jnp.float32)
    gain_two = gain_two_low.astype(jnp.float32)

    wide = group_rows.astype(jnp.float32)
    scale_one = rms_scale(wide)
    normed = (wide * scale_one * gain_one).astype(jnp.bfloat16)
    cosine, sine = rope_tables(segment_row)
    query, key_rows, value_rows, compressed, latent_scale, latent_normed = attention_tables(
        normed, query_full, latent_full, expand_full, gain_lat_low, cosine, sine
    )
    mixed, logsum = attend(query, key_rows, value_rows, segment_row)
    mixed_flat = mixed.reshape(row_count, -1)
    attention_own = scatter_sum(
        jnp.dot(mixed_flat, output_full, preferred_element_type=jnp.float32).astype(jnp.bfloat16),
        "tensor",
    )
    wide_own = tokens.astype(jnp.float32)
    hidden = wide_own + attention_own.astype(jnp.float32)
    scale_two = rms_scale(hidden)
    normed_two_own = (hidden * scale_two * gain_two).astype(jnp.bfloat16)

    cot_group = gather(cotangent, "tensor")
    cot_all = gather(cot_group, "dp").reshape(groups, row_count, width)
    normed_two = gather(normed_two_own, "tensor")
    normed_all = gather(normed_two, "dp").reshape(groups, row_count, width)

    expert_ids = jnp.arange(EXPERTS, dtype=jnp.int32)
    chosen = jnp.any(routes_all[:, :, None] == expert_ids[None, None, :], axis=1)
    logits = jnp.dot(
        normed_all.reshape(groups * row_count, width),
        router_full,
        preferred_element_type=jnp.float32,
    )
    sigm = jnp.where(chosen, jax.nn.sigmoid(logits), 0.0)
    picked_total = jnp.sum(sigm, axis=1, keepdims=True)
    gate_dense = route_scale * sigm / picked_total
    first_expert = place_dp * local_experts
    gate_local = lax.dynamic_slice_in_dim(gate_dense, first_expert, local_experts, 1)
    chosen_local = lax.dynamic_slice_in_dim(
        chosen.astype(jnp.bfloat16), first_expert, local_experts, 1
    ).reshape(groups, row_count, local_experts)
    gate_local = jnp.swapaxes(gate_local.reshape(groups, row_count, local_experts), 1, 2)
    places = jnp.arange(row_count, dtype=jnp.int32)
    below = (places[None, :] < places[:, None]).astype(jnp.bfloat16)
    rank = jnp.einsum("ts,gse->get", below, chosen_local, preferred_element_type=jnp.float32)
    slot = jnp.where(jnp.swapaxes(chosen_local, 1, 2) > 0, rank, -1.0).astype(jnp.int32)
    is_slot = slot[:, :, None, :] == jnp.arange(CAP, dtype=jnp.int32)[None, None, :, None]
    pick = is_slot.astype(jnp.bfloat16).reshape(groups, local_experts * CAP, row_count)
    gate_slot = jnp.sum(jnp.where(is_slot, gate_local[:, :, None, :], 0.0), axis=-1)

    rows = jnp.einsum(
        "gst,gtd->gsd", pick, normed_all, preferred_element_type=jnp.float32
    ).astype(jnp.bfloat16).reshape(groups, local_experts, CAP, width)
    cots = jnp.einsum(
        "gst,gtd->gsd", pick, cot_all, preferred_element_type=jnp.float32
    ).astype(jnp.bfloat16).reshape(groups, local_experts, CAP, width)
    expert_pre = jnp.einsum(
        "sxkd,xdcf->sxkcf", rows, expert_in, preferred_element_type=jnp.float32
    )
    gate_pre, up_pre = (expert_pre[..., 0, :], expert_pre[..., 1, :])
    act = jax.nn.silu(gate_pre) * up_pre
    hid_raw = jnp.einsum("sxkd,xfd->sxkf", cots, expert_out, preferred_element_type=jnp.float32)
    gate_grad_slot = jnp.sum(act * hid_raw, axis=-1)
    act_gated = (act * gate_slot[..., None]).astype(jnp.bfloat16)
    gate_part, up_part = swiglu_grad(hid_raw * gate_slot[..., None], gate_pre, up_pre)
    expert_pre_grad = jnp.stack([gate_part, up_part], axis=-2).astype(jnp.bfloat16)
    back_slots = jnp.einsum(
        "sxkcf,xdcf->sxkd", expert_pre_grad, expert_in, preferred_element_type=jnp.float32
    ).astype(jnp.bfloat16).reshape(groups, local_experts * CAP, width)
    out_slots = jnp.einsum(
        "sxkf,xfd->sxkd", act_gated, expert_out, preferred_element_type=jnp.float32
    ).astype(jnp.bfloat16).reshape(groups, local_experts * CAP, width)
    expert_out_grad = jnp.einsum(
        "sxkf,sxkd->xfd", act_gated, cots, preferred_element_type=jnp.float32
    )
    expert_in_grad = jnp.einsum(
        "sxkd,sxkcf->xdcf", rows, expert_pre_grad, preferred_element_type=jnp.float32
    )
    gate_grad_local = jnp.sum(jnp.where(is_slot, gate_grad_slot[..., None], 0.0), axis=2)
    gate_grad_all = lax.dynamic_update_slice_in_dim(
        jnp.zeros((groups * row_count, 2 * EXPERTS), jnp.bfloat16),
        jnp.swapaxes(gate_grad_local, 1, 2)
        .reshape(groups * row_count, local_experts)
        .astype(jnp.bfloat16),
        first_expert,
        1,
    )

    shared_pre = jnp.einsum(
        "gd,dcf->gcf", normed_two, shared_in_full, preferred_element_type=jnp.float32
    )
    shared_act = (jax.nn.silu(shared_pre[:, 0]) * shared_pre[:, 1]).astype(jnp.bfloat16)
    shared_part = jnp.dot(shared_act, shared_out_full, preferred_element_type=jnp.float32)
    shared_hidden_grad = jnp.dot(cot_group, shared_out_full.T, preferred_element_type=jnp.float32)
    shared_gate_part, shared_up_part = swiglu_grad(
        shared_hidden_grad, shared_pre[:, 0], shared_pre[:, 1]
    )
    shared_pre_grad = jnp.stack([shared_gate_part, shared_up_part], axis=1).astype(jnp.bfloat16)
    shared_out_grad = jnp.dot(shared_act.T, cot_group, preferred_element_type=jnp.float32)
    shared_in_grad = jnp.einsum(
        "gd,gcf->dcf", normed_two, shared_pre_grad, preferred_element_type=jnp.float32
    )
    shared_back = jnp.einsum(
        "gcf,dcf->gd", shared_pre_grad, shared_in_full, preferred_element_type=jnp.float32
    )
    mine = (jnp.arange(groups, dtype=jnp.int32) == place_dp)[:, None, None]

    def combine(slots, shared):
        total = jnp.einsum("gst,gsd->gtd", pick, slots, preferred_element_type=jnp.float32)
        total = total + jnp.where(mine, shared[None], 0.0)
        return total.astype(jnp.bfloat16).reshape(groups * row_count, width)

    back_sum = combine(back_slots, shared_back)
    back_sum = jnp.concatenate([back_sum, gate_grad_all], axis=1)
    back_own = scatter_sum(scatter_sum(back_sum, "dp"), "tensor").astype(jnp.float32)
    out_sum = combine(out_slots, shared_part)
    out_own = scatter_sum(scatter_sum(out_sum, "dp"), "tensor").astype(jnp.float32)
    out_tokens = (hidden + out_own).astype(jnp.bfloat16)

    first_token = place_dp * row_count + first_row
    sigm_own = own_slice(sigm, first_token, own_rows)
    total_own = own_slice(picked_total, first_token, own_rows)
    gate_grad = back_own[:, width : width + EXPERTS]
    picked_grad = route_scale * (
        gate_grad / total_own
        - jnp.sum(gate_grad * sigm_own, axis=1, keepdims=True) / (total_own * total_own)
    )
    logit_grad = picked_grad * sigm_own * (1.0 - sigm_own)
    router_grad = jnp.dot(
        normed_two_own.astype(jnp.float32).T, logit_grad, precision=lax.Precision.HIGHEST
    )
    router_back = jnp.dot(
        logit_grad, router_full.astype(jnp.float32).T, precision=lax.Precision.HIGHEST
    )
    normed_two_grad = back_own[:, :width] + router_back
    weighted_two = normed_two_grad * gain_two
    hidden_grad = (
        cotangent.astype(jnp.float32)
        + scale_two * weighted_two
        - hidden * scale_two**3 * jnp.mean(hidden * weighted_two, axis=-1, keepdims=True)
    )
    gain_two_grad = jnp.sum(normed_two_grad * hidden * scale_two, axis=0)
    hidden_low = gather(hidden_grad.astype(jnp.bfloat16), "tensor")

    output_grad = jnp.dot(mixed_flat.T, hidden_low, preferred_element_type=jnp.float32)
    mixed_grad = (
        jnp.dot(hidden_low, output_full.T, preferred_element_type=jnp.float32)
        .astype(jnp.bfloat16)
        .reshape(mixed.shape)
    )
    query_grad, key_grad, value_grad = attend_back(
        query, key_rows, value_rows, segment_row, mixed_grad, logsum
    )
    query_pre = (
        jnp.concatenate(
            [
                query_grad[..., :DN],
                unrotate(query_grad[..., DN:], cosine[:, None, :], sine[:, None, :]),
            ],
            axis=-1,
        )
        .astype(jnp.bfloat16)
        .reshape(row_count, -1)
    )
    query_grad_weight = jnp.dot(normed.T, query_pre, preferred_element_type=jnp.float32)
    normed_grad = jnp.dot(query_pre, query_full.T, preferred_element_type=jnp.float32)
    keyvalue_grad = (
        jnp.concatenate([key_grad[..., :DN], value_grad], axis=-1)
        .astype(jnp.bfloat16)
        .reshape(row_count, -1)
    )
    expand_grad = jnp.dot(latent_normed.T, keyvalue_grad, preferred_element_type=jnp.float32)
    latent_normed_grad = jnp.dot(keyvalue_grad, expand_full.T, preferred_element_type=jnp.float32)
    rope_grad = unrotate(jnp.sum(key_grad[..., DN:], axis=1), cosine, sine)
    lat_weighted = latent_normed_grad * gain_lat_low.astype(jnp.float32)
    gain_lat_grad = jnp.sum(latent_normed_grad * compressed * latent_scale, axis=0)
    compressed_grad = latent_scale * lat_weighted - compressed * latent_scale**3 * jnp.mean(
        compressed * lat_weighted, axis=-1, keepdims=True
    )
    latent_grad = jnp.concatenate([compressed_grad, rope_grad], axis=-1).astype(jnp.bfloat16)
    latent_grad_weight = jnp.dot(normed.T, latent_grad, preferred_element_type=jnp.float32)
    normed_grad = normed_grad + jnp.dot(
        latent_grad, latent_full.T, preferred_element_type=jnp.float32
    )
    normed_own = scatter_sum(normed_grad.astype(jnp.bfloat16), "tensor").astype(jnp.float32)
    scale_own = own_slice(scale_one, first_row, own_rows)
    weighted_one = normed_own * gain_one
    gain_one_grad = jnp.sum(normed_own * wide_own * scale_own, axis=0)
    tokens_grad = (
        hidden_grad
        + scale_own * weighted_one
        - wide_own * scale_own**3 * jnp.mean(wide_own * weighted_one, axis=-1, keepdims=True)
    )

    shared_out_out = scatter_sum(shared_out_grad.astype(jnp.bfloat16), "dp", 1).astype(jnp.float32)
    shared_in_out = scatter_sum(shared_in_grad.astype(jnp.bfloat16), "dp").astype(jnp.float32)
    output_out = scatter_sum(output_grad.astype(jnp.bfloat16), "dp", 1).astype(jnp.float32)
    expand_out = scatter_sum(expand_grad.astype(jnp.bfloat16), "dp").astype(jnp.float32)
    query_out = scatter_sum(query_grad_weight.astype(jnp.bfloat16), "dp").astype(jnp.float32)
    lat_rows = latent_gain.shape[0]
    gain_rows = attention_gain.shape[0]
    lat_column = jnp.pad(
        gain_lat_grad.reshape(-1, lat_rows), ((0, 0), (0, gain_rows - lat_rows))
    ).reshape(-1)
    columns = jnp.stack([gain_one_grad, gain_two_grad, lat_column], axis=1)
    latent_columns = latent_grad_weight.shape[1]
    small = jnp.concatenate([latent_grad_weight, router_grad, columns], axis=1)
    small = jnp.pad(small, ((0, 0), (0, -small.shape[1] % 128))).astype(jnp.bfloat16)
    small = scatter_sum(scatter_sum(small, "dp"), "tensor").astype(jnp.float32)
    latent_out = small[:, :latent_columns]
    router_out = small[:, latent_columns : latent_columns + EXPERTS]
    last = latent_columns + EXPERTS
    gain_one_out = small[:, last]
    gain_two_out = small[:, last + 1]
    gain_lat_out = small[:lat_rows, last + 2]
    return (
        out_tokens,
        tokens_grad,
        gain_one_out,
        gain_lat_out,
        gain_two_out,
        query_out,
        latent_out,
        expand_out,
        output_out,
        router_out,
        shared_in_out,
        shared_out_out,
        expert_in_grad,
        expert_out_grad,
    )


def solution(mesh):
    placed = (
        P(("dp", "tensor"), None),
        P("dp", None),
        P("dp", None),
        P(("dp", "tensor"), None),
        P(("dp", "tensor")),
        P(("dp", "tensor")),
        P(("dp", "tensor")),
        P("dp", "tensor"),
        P(("dp", "tensor"), None),
        P("dp", "tensor"),
        P("tensor", "dp"),
        P(("dp", "tensor"), None),
        P("dp", None, "tensor"),
        P("tensor", "dp"),
        P("dp", None, None, "tensor"),
        P("dp", "tensor", None),
    )
    return jax.shard_map(
        body,
        mesh=mesh,
        in_specs=placed,
        out_specs=(
            P(("dp", "tensor"), None),
            P(("dp", "tensor"), None),
            P(("dp", "tensor")),
            P(("dp", "tensor")),
            P(("dp", "tensor")),
            P("dp", "tensor"),
            P(("dp", "tensor"), None),
            P("dp", "tensor"),
            P("tensor", "dp"),
            P(("dp", "tensor"), None),
            P("dp", None, "tensor"),
            P("tensor", "dp"),
            P("dp", None, None, "tensor"),
            P("dp", "tensor", None),
        ),
        check_vma=False,
    )
```

```python
import jax
import jax.numpy as jnp
from jax import lax
from jax.experimental import pallas as pl
from jax.experimental.pallas import tpu as pltpu
from jax.sharding import PartitionSpec as P

DN = 128
DR = 64
DV = 128
KVR = 512
EXPERTS = 64
TOPK = 6
CAP = 72
BOTH = ("dp", "tensor")


epsilon = 1e-06
route_scale = 2.446
rope_base = 50000.0
excluded = -1e30


def rms_scale(array_in):
    return lax.rsqrt(jnp.mean(array_in * array_in, axis=-1, keepdims=True) + epsilon)


def rope_tables(segment_row):
    places = jnp.arange(segment_row.shape[0], dtype=jnp.int32)
    begins = jnp.sum((segment_row[None, :] < segment_row[:, None]).astype(jnp.int32), axis=1)
    position = (places - begins).astype(jnp.float32)
    freqs = rope_base ** (-jnp.arange(DR // 2, dtype=jnp.float32) * 2.0 / DR)
    angle = position[:, None] * freqs[None, :]
    return (jnp.cos(angle), jnp.sin(angle))


def rotate(array_in, cosine, sine):
    half_width = array_in.shape[-1] // 2
    first_half, second_half = (array_in[..., :half_width], array_in[..., half_width:])
    return jnp.concatenate(
        [first_half * cosine - second_half * sine, second_half * cosine + first_half * sine],
        axis=-1,
    )


def unrotate(array_in, cosine, sine):
    half_width = array_in.shape[-1] // 2
    first_half, second_half = (array_in[..., :half_width], array_in[..., half_width:])
    return jnp.concatenate(
        [first_half * cosine + second_half * sine, second_half * cosine - first_half * sine],
        axis=-1,
    )


def attention_tables(normed, query_weight, latent_weight, expand_weight, latent_gain, cosine, sine):
    row_count = normed.shape[0]
    head_count = query_weight.shape[1] // (DN + DR)
    query = jnp.dot(normed, query_weight, preferred_element_type=jnp.float32).reshape(
        row_count, head_count, DN + DR
    )
    query = jnp.concatenate(
        [query[..., :DN], rotate(query[..., DN:], cosine[:, None, :], sine[:, None, :])], axis=-1
    ).astype(jnp.bfloat16)
    latent = jnp.dot(normed, latent_weight, preferred_element_type=jnp.float32)
    compressed = latent[:, :KVR]
    latent_scale = rms_scale(compressed)
    latent_normed = (compressed * latent_scale * latent_gain.astype(jnp.float32)).astype(
        jnp.bfloat16
    )
    rope_key = rotate(latent[:, KVR:], cosine, sine)
    keyvalue = jnp.dot(latent_normed, expand_weight, preferred_element_type=jnp.float32).reshape(
        row_count, head_count, DN + DV
    )
    key_rows = jnp.concatenate(
        [keyvalue[..., :DN], jnp.broadcast_to(rope_key[:, None, :], (row_count, head_count, DR))],
        axis=-1,
    ).astype(jnp.bfloat16)
    value_rows = keyvalue[..., DN:].astype(jnp.bfloat16)
    return (query, key_rows, value_rows, compressed, latent_scale, latent_normed)


def masked_scores(query, key_rows, segment_row):
    scores = jnp.einsum(
        "qhd,khd->hqk", query, key_rows, preferred_element_type=jnp.float32
    ) * query.shape[-1] ** (-0.5)
    places = jnp.arange(key_rows.shape[0], dtype=jnp.int32)
    allowed = (segment_row[None, :] == segment_row[:, None]) & (places[None, :] <= places[:, None])
    return jnp.where(allowed[None], scores, excluded)


def attend(query, key_rows, value_rows, segment_row):
    scores = masked_scores(query, key_rows, segment_row)
    logsum = jnp.log(jnp.sum(jnp.exp(scores), axis=-1))
    weights_low = jnp.exp(scores - logsum[..., None]).astype(jnp.bfloat16)
    mixed = jnp.einsum(
        "hqk,khd->qhd", weights_low, value_rows, preferred_element_type=jnp.float32
    ).astype(jnp.bfloat16)
    return (mixed, logsum)


def attend_back(query, key_rows, value_rows, segment_row, out_grad, logsum):
    scores = masked_scores(query, key_rows, segment_row)
    weights_full = jnp.exp(scores - logsum[..., None])
    weights_low = weights_full.astype(jnp.bfloat16)
    prob_grad = jnp.einsum("qhd,khd->hqk", out_grad, value_rows, preferred_element_type=jnp.float32)
    row_total = jnp.sum(weights_full * prob_grad, axis=-1, keepdims=True)
    score_grad = (weights_full * (prob_grad - row_total) * query.shape[-1] ** (-0.5)).astype(
        jnp.bfloat16
    )
    query_grad = jnp.einsum("hqk,khd->qhd", score_grad, key_rows, preferred_element_type=jnp.float32)
    key_grad = jnp.einsum("hqk,qhd->khd", score_grad, query, preferred_element_type=jnp.float32)
    value_grad = jnp.einsum("hqk,qhd->khd", weights_low, out_grad, preferred_element_type=jnp.float32)
    return (query_grad, key_grad, value_grad)


def swiglu_grad(hidden_grad, gate_pre, up_pre):
    sigm = jax.nn.sigmoid(gate_pre)
    return (
        hidden_grad * up_pre * sigm * (1.0 + gate_pre * (1.0 - sigm)),
        hidden_grad * jax.nn.silu(gate_pre),
    )


def gather(array_in, axis_name, axis=0):
    return lax.all_gather(array_in, axis_name, axis=axis, tiled=True)


def scatter_sum(array_in, axis_name, axis=0):
    return lax.psum_scatter(array_in, axis_name, scatter_dimension=axis, tiled=True)


def own_slice(array_in, first_row, own_rows):
    return lax.dynamic_slice_in_dim(array_in, first_row, own_rows, 0)


class Cube:
    def __init__(self, axes):
        self.axes = axes
        self.sizes = {a: lax.axis_size(a) for a in axes}
        self.total = 1
        for a in axes:
            self.total *= self.sizes[a]

    def flat(self, pos):
        index = 0
        for a in self.axes:
            index = index * self.sizes[a] + pos[a]
        return index


def flipped(pos, name, bit):
    value = pos[name]
    has = (value // (1 << bit)) % 2
    new = dict(pos)
    new[name] = value + (1 - 2 * has) * (1 << bit)
    return new


def moved(pos, order, pattern):
    for step, (name, bit) in enumerate(order):
        if (pattern >> step) & 1:
            pos = flipped(pos, name, bit)
    return pos


def axis_bits(name):
    return range(lax.axis_size(name).bit_length() - 1)


def gather_orders(axes):
    far = [("tensor", b) for b in reversed(axis_bits("tensor"))] if "tensor" in axes else []
    if "dp" not in axes:
        return [far, far]
    middle = [("dp", b) for b in list(axis_bits("dp"))[1:]]
    low = [("dp", 0)]
    return [far + middle + low, far + middle[::-1] + low]


def greet(coords, orders):
    partners = sorted({bit for order in orders for bit in order})
    barrier = pltpu.get_barrier_semaphore()
    for name, bit in partners:
        pl.semaphore_signal(
            barrier,
            inc=1,
            device_id={name: flipped(coords, name, bit)[name]},
            device_id_type=pl.DeviceIdType.MESH,
        )
    pl.semaphore_wait(barrier, len(partners))


def part_of(ref, item, part, index):
    rows, cols = item["rows"] // item["parts"], item["cols"]
    if index is None:
        return ref.at[pl.ds(part * rows, rows), :]
    if item["lanes"]:
        return ref.at[pl.ds(part * rows, rows), pl.ds(pl.multiple_of(index * cols, 128), cols)]
    start = index * item["rows"] + part * rows
    return ref.at[pl.ds(pl.multiple_of(start, 8), rows), :]


def side_by_side(stacked, n):
    rows = stacked.shape[0] // n
    return jnp.swapaxes(stacked.reshape(n, rows, -1), 0, 1).reshape(rows, -1)


def stacked_blocks(wide_array, n):
    rows = wide_array.shape[0]
    return jnp.swapaxes(wide_array.reshape(rows, n, -1), 0, 1).reshape(n * rows, -1)


def size_of(axes):
    return Cube(axes).total


def gather_blocks(blocks, collective_id):
    narrow = [lanes and array.shape[1] % 128 != 0 for array, _, lanes, _ in blocks]
    done = cube_gather(
        [(a, axes, lanes and not thin, parts) for (a, axes, lanes, parts), thin in zip(blocks, narrow)],
        collective_id,
    )
    return [
        side_by_side(out, size_of(block[1])) if thin else out
        for out, block, thin in zip(done, blocks, narrow)
    ]


def reduce_blocks(blocks, collective_id):
    ready = []
    for array, axes, lanes, parts in blocks:
        if lanes and (array.shape[1] // size_of(axes)) % 128 != 0:
            array, lanes = stacked_blocks(array, size_of(axes)), False
        ready.append((array, axes, lanes, parts))
    return cube_reduce(ready, collective_id)


def cube_gather(blocks, collective_id):
    items = []
    for array, axes, lanes, parts in blocks:
        cube = Cube(axes)
        items.append(
            dict(
                rows=array.shape[0], cols=array.shape[1], lanes=lanes, parts=parts,
                cube=cube, orders=gather_orders(axes), dtype=array.dtype,
            )
        )
    count = len(items)
    names = [a for a in BOTH if any(a in item["cube"].axes for item in items)]

    def kernel(*refs):
        ins, outs = refs[:count], refs[count : 2 * count]
        sems = refs[2 * count :]
        coords = {a: lax.axis_index(a) for a in names}
        greet(coords, [order for item in items for order in item["orders"]])
        pending = []

        def copy(i, part, step, slot, src, dst):
            name, bit = items[i]["orders"][part][step]
            return pltpu.make_async_remote_copy(
                src_ref=src,
                dst_ref=dst,
                send_sem=sems[3 * i].at[part, slot],
                recv_sem=sems[3 * i + 1].at[part, slot],
                device_id={name: flipped(coords, name, bit)[name]},
                device_id_type=pl.DeviceIdType.MESH,
            )

        def send(i, part, step, pattern, src, pos):
            dst = part_of(outs[i], items[i], part, items[i]["cube"].flat(pos))
            one = copy(i, part, step, (1 << step) - 1 + pattern, src, dst)
            one.start()
            pending.append(one.wait_send)

        depth = [len(item["orders"][0]) for item in items]
        for step in range(max(depth)):
            for i, item in enumerate(items):
                for part in range(item["parts"]):
                    if step < depth[i]:
                        send(i, part, step, 0, part_of(ins[i], item, part, None), coords)
        for i, item in enumerate(items):
            for part in range(item["parts"]):
                own = part_of(outs[i], item, part, item["cube"].flat(coords))
                one = pltpu.make_async_copy(
                    part_of(ins[i], item, part, None), own, sems[3 * i + 2].at[part]
                )
                one.start()
                pending.append(one.wait)
        for step in range(max(depth)):
            for k in range(1 << step):
                for i, item in enumerate(items):
                    if step >= depth[i]:
                        continue
                    for part in range(item["parts"]):
                        pattern = k + (1 << step)
                        pos = moved(coords, item["orders"][part], pattern)
                        here = part_of(outs[i], item, part, item["cube"].flat(pos))
                        copy(i, part, step, pattern - 1, here, here).wait_recv()
                        for later in range(step + 1, depth[i]):
                            send(i, part, later, pattern, here, pos)
        for wait in pending:
            wait()

    shapes, scratch = [], []
    for item in items:
        n = item["cube"].total
        whole = (item["rows"], item["cols"] * n) if item["lanes"] else (item["rows"] * n, item["cols"])
        shapes.append(jax.ShapeDtypeStruct(whole, item["dtype"]))
        scratch += [pltpu.SemaphoreType.DMA((item["parts"], n - 1))] * 2
        scratch.append(pltpu.SemaphoreType.DMA((item["parts"],)))
    moved_bytes = sum(s.size * s.dtype.itemsize for s in shapes)
    return pl.pallas_call(
        kernel,
        out_shape=shapes,
        in_specs=[pl.BlockSpec(memory_space=pltpu.VMEM)] * count,
        out_specs=[pl.BlockSpec(memory_space=pl.ANY)] * count,
        scratch_shapes=scratch,
        compiler_params=pltpu.CompilerParams(collective_id=collective_id, has_side_effects=True),
        cost_estimate=pl.CostEstimate(flops=0, bytes_accessed=8 * moved_bytes, transcendentals=0),
        name="cube_gather",
    )(*[block[0] for block in blocks])


def cube_reduce(blocks, collective_id):
    items = []
    for array, axes, lanes, parts in blocks:
        cube = Cube(axes)
        rows, cols = array.shape
        rows, cols = (rows, cols // cube.total) if lanes else (rows // cube.total, cols)
        orders = [order[::-1] for order in gather_orders(axes)]
        items.append(
            dict(rows=rows, cols=cols, lanes=lanes, parts=parts, cube=cube, orders=orders, dtype=array.dtype)
        )
    count = len(items)
    names = [a for a in BOTH if any(a in item["cube"].axes for item in items)]

    def kernel(*refs):
        ins, outs = refs[:count], refs[count : 2 * count]
        scratch = refs[2 * count :]
        coords = {a: lax.axis_index(a) for a in names}
        held = [scratch[5 * i] for i in range(count)]
        came = [scratch[5 * i + 1] for i in range(count)]
        send_sem = [scratch[5 * i + 2] for i in range(count)]
        recv_sem = [scratch[5 * i + 3] for i in range(count)]
        load_sem = [scratch[5 * i + 4] for i in range(count)]
        depth = [len(item["orders"][0]) for item in items]
        pending = []

        def load(i, part, k):
            item = items[i]
            pos = moved(coords, item["orders"][part], k << 1)
            return pltpu.make_async_copy(
                part_of(ins[i], item, part, item["cube"].flat(pos)),
                held[i].at[part, k],
                load_sem[i].at[part, k],
            )

        for i, item in enumerate(items):
            for part in range(item["parts"]):
                for k in range(1 << (depth[i] - 1)):
                    load(i, part, k).start()
        greet(coords, [order for item in items for order in item["orders"]])

        def base(i, step):
            return (1 << depth[i]) - (1 << (depth[i] - step))

        def copy(i, part, step, k, src):
            name, bit = items[i]["orders"][part][step]
            slot = base(i, step) + k
            return pltpu.make_async_remote_copy(
                src_ref=src,
                dst_ref=came[i].at[part, slot],
                send_sem=send_sem[i].at[part, slot],
                recv_sem=recv_sem[i].at[part, slot],
                device_id={name: flipped(coords, name, bit)[name]},
                device_id_type=pl.DeviceIdType.MESH,
            )

        def first(count_bits):
            return sorted(range(1 << count_bits), key=lambda k: -(k & 1))

        for i, item in enumerate(items):
            for k in first(depth[i] - 1):
                for part in range(item["parts"]):
                    pos = moved(coords, item["orders"][part], (k << 1) | 1)
                    one = copy(i, part, 0, k, part_of(ins[i], item, part, item["cube"].flat(pos)))
                    one.start()
                    pending.append(one.wait_send)

        def add_up(i, part, pattern, steps, store):
            item = items[i]
            rows = item["rows"] // item["parts"]
            load(i, part, pattern >> 1).wait()
            for step in range(steps):
                k = pattern >> (step + 1)
                copy(i, part, step, k, came[i].at[part, base(i, step) + k]).wait_recv()
            chunk = 16 if rows % 16 == 0 else 8

            def one_chunk(c, carry):
                where = pl.ds(pl.multiple_of(c * chunk, chunk), chunk)
                total = held[i][part, pattern >> 1, where, :].astype(jnp.float32)
                for step in range(steps):
                    slot = base(i, step) + (pattern >> (step + 1))
                    total = total + came[i][part, slot, where, :].astype(jnp.float32)
                store(where, total)
                return carry

            lax.fori_loop(0, rows // chunk, one_chunk, 0)

        for step in range(1, max(depth)):
            for i, item in enumerate(items):
                if step >= depth[i]:
                    continue
                for k in first(depth[i] - step - 1):
                    for part in range(item["parts"]):
                        pattern = ((k << 1) | 1) << step

                        def keep(where, total, i=i, part=part, pattern=pattern):
                            held[i][part, pattern >> 1, where, :] = total.astype(held[i].dtype)

                        add_up(i, part, pattern, step, keep)
                        one = copy(i, part, step, k, held[i].at[part, pattern >> 1])
                        one.start()
                        pending.append(one.wait_send)
        for i, item in enumerate(items):
            rows = item["rows"] // item["parts"]
            for part in range(item["parts"]):

                def put(where, total, i=i, part=part, rows=rows):
                    whole = pl.ds(pl.multiple_of(part * rows + where.start, 8), where.size)
                    outs[i][whole, :] = total

                add_up(i, part, 0, depth[i], put)
        for wait in pending:
            wait()

    shapes, scratch = [], []
    for item in items:
        n = item["cube"].total
        block = (item["rows"] // item["parts"], item["cols"])
        shapes.append(jax.ShapeDtypeStruct((item["rows"], item["cols"]), jnp.float32))
        scratch.append(pltpu.VMEM((item["parts"], n // 2) + block, item["dtype"]))
        scratch.append(pltpu.VMEM((item["parts"], n - 1) + block, item["dtype"]))
        scratch += [pltpu.SemaphoreType.DMA((item["parts"], n - 1))] * 2
        scratch.append(pltpu.SemaphoreType.DMA((item["parts"], n // 2)))
    moved_bytes = sum(block[0].size * block[0].dtype.itemsize for block in blocks)
    return pl.pallas_call(
        kernel,
        out_shape=shapes,
        in_specs=[pl.BlockSpec(memory_space=pl.ANY)] * count,
        out_specs=[pl.BlockSpec(memory_space=pltpu.VMEM)] * count,
        scratch_shapes=scratch,
        compiler_params=pltpu.CompilerParams(
            collective_id=collective_id, has_side_effects=True, vmem_limit_bytes=60 << 20
        ),
        cost_estimate=pl.CostEstimate(flops=0, bytes_accessed=8 * moved_bytes, transcendentals=0),
        name="cube_reduce",
    )(*[block[0] for block in blocks])


def halves(rows):
    return 2 if rows % 32 == 0 else 1


def body(
    tokens,
    segments,
    routes,
    cotangent,
    attention_gain,
    latent_gain,
    feedforward_gain,
    query_weight,
    latent_weight,
    expand_weight,
    output_weight,
    router_weight,
    shared_in,
    shared_out,
    expert_in,
    expert_out,
):
    own_rows, width = tokens.shape
    groups = lax.axis_size("dp")
    place_dp = lax.axis_index("dp")
    first_row = lax.axis_index("tensor") * own_rows
    local_experts = expert_in.shape[0]
    segment_row = segments[0]
    gain_rows, lat_rows = attention_gain.shape[0], latent_gain.shape[0]
    columns = jnp.stack(
        [attention_gain, feedforward_gain, jnp.pad(latent_gain, (0, gain_rows - lat_rows))], axis=1
    )
    router_block = jnp.concatenate([router_weight, columns], axis=1)
    router_block = jnp.pad(router_block, ((0, 0), (0, -router_block.shape[1] % 128)))
    routes_block = jnp.pad(routes.T, ((0, -routes.shape[1] % 8), (0, 0)), constant_values=-1)
    (
        group_rows,
        cot_group,
        latent_full,
        query_full,
        expand_full,
        router_block_full,
        routes_full,
        output_full,
    ) = gather_blocks(
        [
            (tokens, ("tensor",), False, halves(own_rows)),
            (cotangent, ("tensor",), False, halves(own_rows)),
            (latent_weight, BOTH, False, halves(latent_weight.shape[0])),
            (query_weight, ("dp",), False, halves(query_weight.shape[0])),
            (expand_weight, ("dp",), False, halves(expand_weight.shape[0])),
            (router_block, BOTH, False, halves(router_block.shape[0])),
            (routes_block, ("dp",), True, 1),
            (output_weight, ("dp",), True, halves(output_weight.shape[0])),
        ],
        0,
    )
    row_count = group_rows.shape[0]
    router_full = router_block_full[:, :EXPERTS]
    gain_one = router_block_full[:, EXPERTS].astype(jnp.float32)
    gain_two = router_block_full[:, EXPERTS + 1].astype(jnp.float32)
    gain_lat_low = router_block_full[:, EXPERTS + 2].reshape(-1, gain_rows)[:, :lat_rows].reshape(-1)
    routes_all = routes_full[: routes.shape[1]]
    cot_all = gather(cot_group, "dp").reshape(groups, row_count, width)

    wide = group_rows.astype(jnp.float32)
    scale_one = rms_scale(wide)
    normed = (wide * scale_one * gain_one).astype(jnp.bfloat16)
    cosine, sine = rope_tables(segment_row)
    query, key_rows, value_rows, compressed, latent_scale, latent_normed = attention_tables(
        normed, query_full, latent_full, expand_full, gain_lat_low, cosine, sine
    )
    mixed, logsum = attend(query, key_rows, value_rows, segment_row)
    mixed_flat = mixed.reshape(row_count, -1)
    attention_part = jnp.dot(mixed_flat, output_full, preferred_element_type=jnp.float32)
    (attention_own,) = reduce_blocks(
        [(attention_part.astype(jnp.bfloat16), ("tensor",), False, halves(own_rows))], 1
    )
    wide_own = tokens.astype(jnp.float32)
    hidden = wide_own + attention_own
    scale_two = rms_scale(hidden)
    normed_two_own = (hidden * scale_two * gain_two).astype(jnp.bfloat16)

    normed_two_own, cot_all = lax.optimization_barrier((normed_two_own, cot_all))
    (normed_flat,) = gather_blocks([(normed_two_own, BOTH, False, halves(own_rows))], 2)
    normed_flat, shared_in, shared_out = lax.optimization_barrier(
        (normed_flat, shared_in, shared_out)
    )
    shared_in_full = gather(shared_in, "dp")
    shared_out_full = gather(shared_out, "dp", 1)
    normed_all = normed_flat.reshape(groups, row_count, width)
    normed_two = lax.dynamic_index_in_dim(normed_all, place_dp, 0, keepdims=False)

    expert_ids = jnp.arange(EXPERTS, dtype=jnp.int32)
    chosen = jnp.any(routes_all[:, :, None] == expert_ids[None, None, :], axis=0)
    logits = jnp.dot(normed_flat, router_full, preferred_element_type=jnp.float32)
    sigm = jnp.where(chosen, jax.nn.sigmoid(logits), 0.0)
    picked_total = jnp.sum(sigm, axis=1, keepdims=True)
    gate_dense = route_scale * sigm / picked_total
    first_expert = place_dp * local_experts
    gate_local = lax.dynamic_slice_in_dim(gate_dense, first_expert, local_experts, 1)
    chosen_local = lax.dynamic_slice_in_dim(
        chosen.astype(jnp.bfloat16), first_expert, local_experts, 1
    ).reshape(groups, row_count, local_experts)
    gate_local = jnp.swapaxes(gate_local.reshape(groups, row_count, local_experts), 1, 2)
    places = jnp.arange(row_count, dtype=jnp.int32)
    below = (places[None, :] < places[:, None]).astype(jnp.bfloat16)
    rank = jnp.einsum("ts,gse->get", below, chosen_local, preferred_element_type=jnp.float32)
    slot = jnp.where(jnp.swapaxes(chosen_local, 1, 2) > 0, rank, -1.0).astype(jnp.int32)
    is_slot = slot[:, :, None, :] == jnp.arange(CAP, dtype=jnp.int32)[None, None, :, None]
    pick = is_slot.astype(jnp.bfloat16).reshape(groups, local_experts * CAP, row_count)
    gate_slot = jnp.sum(jnp.where(is_slot, gate_local[:, :, None, :], 0.0), axis=-1)

    rows = jnp.einsum(
        "gst,gtd->gsd", pick, normed_all, preferred_element_type=jnp.float32
    ).astype(jnp.bfloat16).reshape(groups, local_experts, CAP, width)
    cots = jnp.einsum(
        "gst,gtd->gsd", pick, cot_all, preferred_element_type=jnp.float32
    ).astype(jnp.bfloat16).reshape(groups, local_experts, CAP, width)
    expert_pre = jnp.einsum(
        "sxkd,xdcf->sxkcf", rows, expert_in, preferred_element_type=jnp.float32
    )
    gate_pre, up_pre = (expert_pre[..., 0, :], expert_pre[..., 1, :])
    act = jax.nn.silu(gate_pre) * up_pre
    hid_raw = jnp.einsum("sxkd,xfd->sxkf", cots, expert_out, preferred_element_type=jnp.float32)
    gate_grad_slot = jnp.sum(act * hid_raw, axis=-1)
    act_gated = (act * gate_slot[..., None]).astype(jnp.bfloat16)
    gate_part, up_part = swiglu_grad(hid_raw * gate_slot[..., None], gate_pre, up_pre)
    expert_pre_grad = jnp.stack([gate_part, up_part], axis=-2).astype(jnp.bfloat16)
    back_slots = jnp.einsum(
        "sxkcf,xdcf->sxkd", expert_pre_grad, expert_in, preferred_element_type=jnp.float32
    ).astype(jnp.bfloat16).reshape(groups, local_experts * CAP, width)
    out_slots = jnp.einsum(
        "sxkf,xfd->sxkd", act_gated, expert_out, preferred_element_type=jnp.float32
    ).astype(jnp.bfloat16).reshape(groups, local_experts * CAP, width)
    expert_out_grad = jnp.einsum(
        "sxkf,sxkd->xfd", act_gated, cots, preferred_element_type=jnp.float32
    )
    expert_in_grad = jnp.einsum(
        "sxkd,sxkcf->xdcf", rows, expert_pre_grad, preferred_element_type=jnp.float32
    )
    gate_grad_local = jnp.sum(jnp.where(is_slot, gate_grad_slot[..., None], 0.0), axis=2)
    gate_grad_all = lax.dynamic_update_slice_in_dim(
        jnp.zeros((groups * row_count, 2 * EXPERTS), jnp.bfloat16),
        jnp.swapaxes(gate_grad_local, 1, 2)
        .reshape(groups * row_count, local_experts)
        .astype(jnp.bfloat16),
        first_expert,
        1,
    )

    shared_pre = jnp.einsum(
        "gd,dcf->gcf", normed_two, shared_in_full, preferred_element_type=jnp.float32
    )
    shared_act = (jax.nn.silu(shared_pre[:, 0]) * shared_pre[:, 1]).astype(jnp.bfloat16)
    shared_part = jnp.dot(shared_act, shared_out_full, preferred_element_type=jnp.float32)
    shared_hidden_grad = jnp.dot(cot_group, shared_out_full.T, preferred_element_type=jnp.float32)
    shared_gate_part, shared_up_part = swiglu_grad(
        shared_hidden_grad, shared_pre[:, 0], shared_pre[:, 1]
    )
    shared_pre_grad = jnp.stack([shared_gate_part, shared_up_part], axis=1).astype(jnp.bfloat16)
    shared_out_grad = jnp.dot(
        shared_act.T, cot_group, preferred_element_type=jnp.float32
    ).astype(jnp.bfloat16)
    shared_in_grad = jnp.einsum(
        "gcf,gd->cfd", shared_pre_grad, normed_two, preferred_element_type=jnp.float32
    ).astype(jnp.bfloat16)
    shared_back = jnp.einsum(
        "gcf,dcf->gd", shared_pre_grad, shared_in_full, preferred_element_type=jnp.float32
    )
    mine = (jnp.arange(groups, dtype=jnp.int32) == place_dp)[:, None, None]

    def combine(slots, shared):
        total = jnp.einsum("gst,gsd->gtd", pick, slots, preferred_element_type=jnp.float32)
        total = total + jnp.where(mine, shared[None], 0.0)
        return total.astype(jnp.bfloat16).reshape(groups * row_count, width)

    back_sum = combine(back_slots, shared_back)
    back_group = scatter_sum(back_sum, "dp")
    out_sum = combine(out_slots, shared_part)
    (
        back_group,
        out_sum,
        expert_out_grad,
        expert_in_grad,
        shared_out_grad,
        shared_in_grad,
        gate_grad_all,
    ) = lax.optimization_barrier(
        (
            back_group,
            out_sum,
            expert_out_grad,
            expert_in_grad,
            shared_out_grad,
            shared_in_grad,
            gate_grad_all,
        )
    )
    back_own, gate_grad_own = reduce_blocks(
        [
            (back_group, ("tensor",), False, halves(own_rows)),
            (gate_grad_all, BOTH, False, 1),
        ],
        3,
    )
    out_group = scatter_sum(out_sum, "dp")

    first_token = place_dp * row_count + first_row
    sigm_own = own_slice(sigm, first_token, own_rows)
    total_own = own_slice(picked_total, first_token, own_rows)
    gate_grad = gate_grad_own[:, :EXPERTS]
    picked_grad = route_scale * (
        gate_grad / total_own
        - jnp.sum(gate_grad * sigm_own, axis=1, keepdims=True) / (total_own * total_own)
    )
    logit_grad = picked_grad * sigm_own * (1.0 - sigm_own)
    router_grad = jnp.dot(
        normed_two_own.astype(jnp.float32).T, logit_grad, precision=lax.Precision.HIGHEST
    )
    router_back = jnp.dot(
        logit_grad, router_full.astype(jnp.float32).T, precision=lax.Precision.HIGHEST
    )
    normed_two_grad = back_own + router_back
    weighted_two = normed_two_grad * gain_two
    hidden_grad = (
        cotangent.astype(jnp.float32)
        + scale_two * weighted_two
        - hidden * scale_two**3 * jnp.mean(hidden * weighted_two, axis=-1, keepdims=True)
    )
    gain_two_grad = jnp.sum(normed_two_grad * hidden * scale_two, axis=0)
    (hidden_low,) = gather_blocks(
        [(hidden_grad.astype(jnp.bfloat16), ("tensor",), False, halves(own_rows))], 4
    )

    output_grad = jnp.dot(mixed_flat.T, hidden_low, preferred_element_type=jnp.float32)
    mixed_grad = (
        jnp.dot(hidden_low, output_full.T, preferred_element_type=jnp.float32)
        .astype(jnp.bfloat16)
        .reshape(mixed.shape)
    )
    query_grad, key_grad, value_grad = attend_back(
        query, key_rows, value_rows, segment_row, mixed_grad, logsum
    )
    query_pre = (
        jnp.concatenate(
            [
                query_grad[..., :DN],
                unrotate(query_grad[..., DN:], cosine[:, None, :], sine[:, None, :]),
            ],
            axis=-1,
        )
        .astype(jnp.bfloat16)
        .reshape(row_count, -1)
    )
    query_pre, out_group = lax.optimization_barrier((query_pre, out_group))
    out_own = scatter_sum(out_group, "tensor").astype(jnp.float32)
    query_grad_weight = jnp.dot(normed.T, query_pre, preferred_element_type=jnp.float32)
    normed_grad = jnp.dot(query_pre, query_full.T, preferred_element_type=jnp.float32)
    keyvalue_grad = (
        jnp.concatenate([key_grad[..., :DN], value_grad], axis=-1)
        .astype(jnp.bfloat16)
        .reshape(row_count, -1)
    )
    expand_grad = jnp.dot(latent_normed.T, keyvalue_grad, preferred_element_type=jnp.float32)
    latent_normed_grad = jnp.dot(keyvalue_grad, expand_full.T, preferred_element_type=jnp.float32)
    rope_grad = unrotate(jnp.sum(key_grad[..., DN:], axis=1), cosine, sine)
    lat_weighted = latent_normed_grad * gain_lat_low.astype(jnp.float32)
    gain_lat_grad = jnp.sum(latent_normed_grad * compressed * latent_scale, axis=0)
    compressed_grad = latent_scale * lat_weighted - compressed * latent_scale**3 * jnp.mean(
        compressed * lat_weighted, axis=-1, keepdims=True
    )
    latent_grad = jnp.concatenate([compressed_grad, rope_grad], axis=-1).astype(jnp.bfloat16)
    latent_grad_weight = jnp.dot(normed.T, latent_grad, preferred_element_type=jnp.float32)
    normed_grad = normed_grad + jnp.dot(
        latent_grad, latent_full.T, preferred_element_type=jnp.float32
    )
    gain_one_grad = jnp.sum(normed_grad * wide * scale_one, axis=0)

    lat_column = jnp.pad(
        gain_lat_grad.reshape(-1, lat_rows), ((0, 0), (0, gain_rows - lat_rows))
    ).reshape(-1)
    columns = jnp.stack([gain_one_grad, gain_two_grad, lat_column], axis=1).astype(jnp.bfloat16)
    latent_columns = latent_grad_weight.shape[1]
    small = jnp.concatenate(
        [latent_grad_weight.astype(jnp.bfloat16), router_grad.astype(jnp.bfloat16), columns], axis=1
    )
    small = jnp.pad(small, ((0, 0), (0, -small.shape[1] % 128)))
    hidden_units = shared_in.shape[2]
    normed_own, query_out, expand_out, output_out, shared_in_out, shared_out_out, small = (
        reduce_blocks(
            [
                (normed_grad.astype(jnp.bfloat16), ("tensor",), False, halves(own_rows)),
                (
                    query_grad_weight.astype(jnp.bfloat16),
                    ("dp",),
                    False,
                    halves(query_weight.shape[0]),
                ),
                (expand_grad.astype(jnp.bfloat16), ("dp",), False, halves(expand_weight.shape[0])),
                (output_grad.astype(jnp.bfloat16), ("dp",), True, halves(output_weight.shape[0])),
                (
                    shared_in_grad.reshape(2 * hidden_units, width),
                    ("dp",),
                    True,
                    halves(2 * hidden_units),
                ),
                (shared_out_grad, ("dp",), True, halves(hidden_units)),
                (small, BOTH, False, 1),
            ],
            5,
        )
    )
    shared_in_out = jnp.moveaxis(shared_in_out.reshape(2, hidden_units, -1), 2, 0)
    latent_out = small[:, :latent_columns]
    router_out = small[:, latent_columns : latent_columns + EXPERTS]
    last = latent_columns + EXPERTS
    gain_one_out = small[:, last]
    gain_two_out = small[:, last + 1]
    gain_lat_out = small[:lat_rows, last + 2]
    scale_own = own_slice(scale_one, first_row, own_rows)
    weighted_one = normed_own * gain_one
    tokens_grad = (
        hidden_grad
        + scale_own * weighted_one
        - wide_own * scale_own**3 * jnp.mean(wide_own * weighted_one, axis=-1, keepdims=True)
    )
    out_tokens = (hidden + out_own).astype(jnp.bfloat16)
    return (
        out_tokens,
        tokens_grad,
        gain_one_out,
        gain_lat_out,
        gain_two_out,
        query_out,
        latent_out,
        expand_out,
        output_out,
        router_out,
        shared_in_out,
        shared_out_out,
        expert_in_grad,
        expert_out_grad,
    )


def solution(mesh):
    placed = (
        P(("dp", "tensor"), None),
        P("dp", None),
        P("dp", None),
        P(("dp", "tensor"), None),
        P(("dp", "tensor")),
        P(("dp", "tensor")),
        P(("dp", "tensor")),
        P("dp", "tensor"),
        P(("dp", "tensor"), None),
        P("dp", "tensor"),
        P("tensor", "dp"),
        P(("dp", "tensor"), None),
        P("dp", None, "tensor"),
        P("tensor", "dp"),
        P("dp", None, None, "tensor"),
        P("dp", "tensor", None),
    )
    return jax.shard_map(
        body,
        mesh=mesh,
        in_specs=placed,
        out_specs=(
            P(("dp", "tensor"), None),
            P(("dp", "tensor"), None),
            P(("dp", "tensor")),
            P(("dp", "tensor")),
            P(("dp", "tensor")),
            P("dp", "tensor"),
            P(("dp", "tensor"), None),
            P("dp", "tensor"),
            P("tensor", "dp"),
            P(("dp", "tensor"), None),
            P("dp", None, "tensor"),
            P("tensor", "dp"),
            P("dp", None, None, "tensor"),
            P("dp", "tensor", None),
        ),
        check_vma=False,
    )
```

```python
import jax
import jax.numpy as jnp
from jax import lax
from jax.experimental import pallas as pl
from jax.experimental.pallas import tpu as pltpu
from jax.sharding import PartitionSpec as P

DN = 128
DR = 64
DV = 128
KVR = 512
EXPERTS = 64
TOPK = 6
CAP = 72
BOTH = ("dp", "tensor")


epsilon = 1e-06
route_scale = 2.446
rope_base = 50000.0
excluded = -1e30


def rms_scale(array_in):
    return lax.rsqrt(jnp.mean(array_in * array_in, axis=-1, keepdims=True) + epsilon)


def rope_tables(segment_row):
    places = jnp.arange(segment_row.shape[0], dtype=jnp.int32)
    begins = jnp.sum((segment_row[None, :] < segment_row[:, None]).astype(jnp.int32), axis=1)
    position = (places - begins).astype(jnp.float32)
    freqs = rope_base ** (-jnp.arange(DR // 2, dtype=jnp.float32) * 2.0 / DR)
    angle = position[:, None] * freqs[None, :]
    return (jnp.cos(angle), jnp.sin(angle))


def rotate(array_in, cosine, sine):
    half_width = array_in.shape[-1] // 2
    first_half, second_half = (array_in[..., :half_width], array_in[..., half_width:])
    return jnp.concatenate(
        [first_half * cosine - second_half * sine, second_half * cosine + first_half * sine],
        axis=-1,
    )


def unrotate(array_in, cosine, sine):
    half_width = array_in.shape[-1] // 2
    first_half, second_half = (array_in[..., :half_width], array_in[..., half_width:])
    return jnp.concatenate(
        [first_half * cosine + second_half * sine, second_half * cosine - first_half * sine],
        axis=-1,
    )


def attention_tables(normed, query_weight, latent_weight, expand_weight, latent_gain, cosine, sine):
    row_count = normed.shape[0]
    head_count = query_weight.shape[1] // (DN + DR)
    query = jnp.dot(normed, query_weight, preferred_element_type=jnp.float32).reshape(
        row_count, head_count, DN + DR
    )
    query = jnp.concatenate(
        [query[..., :DN], rotate(query[..., DN:], cosine[:, None, :], sine[:, None, :])], axis=-1
    ).astype(jnp.bfloat16)
    latent = jnp.dot(normed, latent_weight, preferred_element_type=jnp.float32)
    compressed = latent[:, :KVR]
    latent_scale = rms_scale(compressed)
    latent_normed = (compressed * latent_scale * latent_gain.astype(jnp.float32)).astype(
        jnp.bfloat16
    )
    rope_key = rotate(latent[:, KVR:], cosine, sine)
    keyvalue = jnp.dot(latent_normed, expand_weight, preferred_element_type=jnp.float32).reshape(
        row_count, head_count, DN + DV
    )
    key_rows = jnp.concatenate(
        [keyvalue[..., :DN], jnp.broadcast_to(rope_key[:, None, :], (row_count, head_count, DR))],
        axis=-1,
    ).astype(jnp.bfloat16)
    value_rows = keyvalue[..., DN:].astype(jnp.bfloat16)
    return (query, key_rows, value_rows, compressed, latent_scale, latent_normed)


def masked_scores(query, key_rows, segment_row):
    scores = jnp.einsum(
        "qhd,khd->hqk", query, key_rows, preferred_element_type=jnp.float32
    ) * query.shape[-1] ** (-0.5)
    places = jnp.arange(key_rows.shape[0], dtype=jnp.int32)
    allowed = (segment_row[None, :] == segment_row[:, None]) & (places[None, :] <= places[:, None])
    return jnp.where(allowed[None], scores, excluded)


def attend(query, key_rows, value_rows, segment_row):
    scores = masked_scores(query, key_rows, segment_row)
    logsum = jnp.log(jnp.sum(jnp.exp(scores), axis=-1))
    weights_low = jnp.exp(scores - logsum[..., None]).astype(jnp.bfloat16)
    mixed = jnp.einsum(
        "hqk,khd->qhd", weights_low, value_rows, preferred_element_type=jnp.float32
    ).astype(jnp.bfloat16)
    return (mixed, logsum)


def attend_back(query, key_rows, value_rows, segment_row, out_grad, logsum):
    scores = masked_scores(query, key_rows, segment_row)
    weights_full = jnp.exp(scores - logsum[..., None])
    weights_low = weights_full.astype(jnp.bfloat16)
    prob_grad = jnp.einsum("qhd,khd->hqk", out_grad, value_rows, preferred_element_type=jnp.float32)
    row_total = jnp.sum(weights_full * prob_grad, axis=-1, keepdims=True)
    score_grad = (weights_full * (prob_grad - row_total) * query.shape[-1] ** (-0.5)).astype(
        jnp.bfloat16
    )
    query_grad = jnp.einsum("hqk,khd->qhd", score_grad, key_rows, preferred_element_type=jnp.float32)
    key_grad = jnp.einsum("hqk,qhd->khd", score_grad, query, preferred_element_type=jnp.float32)
    value_grad = jnp.einsum("hqk,qhd->khd", weights_low, out_grad, preferred_element_type=jnp.float32)
    return (query_grad, key_grad, value_grad)


def swiglu_grad(hidden_grad, gate_pre, up_pre):
    sigm = jax.nn.sigmoid(gate_pre)
    return (
        hidden_grad * up_pre * sigm * (1.0 + gate_pre * (1.0 - sigm)),
        hidden_grad * jax.nn.silu(gate_pre),
    )


def gather(array_in, axis_name, axis=0):
    return lax.all_gather(array_in, axis_name, axis=axis, tiled=True)


def scatter_sum(array_in, axis_name, axis=0):
    return lax.psum_scatter(array_in, axis_name, scatter_dimension=axis, tiled=True)


def own_slice(array_in, first_row, own_rows):
    return lax.dynamic_slice_in_dim(array_in, first_row, own_rows, 0)


class Cube:
    def __init__(self, axes):
        self.axes = axes
        self.sizes = {a: lax.axis_size(a) for a in axes}
        self.total = 1
        for a in axes:
            self.total *= self.sizes[a]

    def flat(self, pos):
        index = 0
        for a in self.axes:
            index = index * self.sizes[a] + pos[a]
        return index


def flipped(pos, name, bit):
    value = pos[name]
    has = (value // (1 << bit)) % 2
    new = dict(pos)
    new[name] = value + (1 - 2 * has) * (1 << bit)
    return new


def moved(pos, order, pattern):
    for step, (name, bit) in enumerate(order):
        if (pattern >> step) & 1:
            pos = flipped(pos, name, bit)
    return pos


def axis_bits(name):
    return range(lax.axis_size(name).bit_length() - 1)


def gather_orders(axes):
    far = [("tensor", b) for b in reversed(axis_bits("tensor"))] if "tensor" in axes else []
    if "dp" not in axes:
        return [far, far]
    middle = [("dp", b) for b in list(axis_bits("dp"))[1:]]
    low = [("dp", 0)]
    return [far + middle + low, far + middle[::-1] + low]


def greet(coords, orders):
    partners = sorted({bit for order in orders for bit in order})
    barrier = pltpu.get_barrier_semaphore()
    for name, bit in partners:
        pl.semaphore_signal(
            barrier,
            inc=1,
            device_id={name: flipped(coords, name, bit)[name]},
            device_id_type=pl.DeviceIdType.MESH,
        )
    pl.semaphore_wait(barrier, len(partners))


def part_of(ref, item, part, index):
    rows, cols = item["rows"] // item["parts"], item["cols"]
    if index is None:
        return ref.at[pl.ds(part * rows, rows), :]
    if item["lanes"]:
        return ref.at[pl.ds(part * rows, rows), pl.ds(pl.multiple_of(index * cols, 128), cols)]
    start = index * item["rows"] + part * rows
    return ref.at[pl.ds(pl.multiple_of(start, 8), rows), :]


def side_by_side(stacked, n):
    rows = stacked.shape[0] // n
    return jnp.swapaxes(stacked.reshape(n, rows, -1), 0, 1).reshape(rows, -1)


def stacked_blocks(wide_array, n):
    rows = wide_array.shape[0]
    return jnp.swapaxes(wide_array.reshape(rows, n, -1), 0, 1).reshape(n * rows, -1)


def size_of(axes):
    return Cube(axes).total


def gather_blocks(blocks, collective_id):
    narrow = [lanes and array.shape[1] % 128 != 0 for array, _, lanes, _ in blocks]
    done = cube_gather(
        [(a, axes, lanes and not thin, parts) for (a, axes, lanes, parts), thin in zip(blocks, narrow)],
        collective_id,
    )
    return [
        side_by_side(out, size_of(block[1])) if thin else out
        for out, block, thin in zip(done, blocks, narrow)
    ]


def reduce_blocks(blocks, collective_id):
    ready = []
    for array, axes, lanes, parts in blocks:
        if lanes and (array.shape[1] // size_of(axes)) % 128 != 0:
            array, lanes = stacked_blocks(array, size_of(axes)), False
        ready.append((array, axes, lanes, parts))
    return cube_reduce(ready, collective_id)


def cube_gather(blocks, collective_id):
    items = []
    for array, axes, lanes, parts in blocks:
        cube = Cube(axes)
        items.append(
            dict(
                rows=array.shape[0], cols=array.shape[1], lanes=lanes, parts=parts,
                cube=cube, orders=gather_orders(axes), dtype=array.dtype,
            )
        )
    count = len(items)
    names = [a for a in BOTH if any(a in item["cube"].axes for item in items)]

    def kernel(*refs):
        ins, outs = refs[:count], refs[count : 2 * count]
        sems = refs[2 * count :]
        coords = {a: lax.axis_index(a) for a in names}
        greet(coords, [order for item in items for order in item["orders"]])
        pending = []

        def copy(i, part, step, slot, src, dst):
            name, bit = items[i]["orders"][part][step]
            return pltpu.make_async_remote_copy(
                src_ref=src,
                dst_ref=dst,
                send_sem=sems[3 * i].at[part, slot],
                recv_sem=sems[3 * i + 1].at[part, slot],
                device_id={name: flipped(coords, name, bit)[name]},
                device_id_type=pl.DeviceIdType.MESH,
            )

        def send(i, part, step, pattern, src, pos):
            dst = part_of(outs[i], items[i], part, items[i]["cube"].flat(pos))
            one = copy(i, part, step, (1 << step) - 1 + pattern, src, dst)
            one.start()
            pending.append(one.wait_send)

        depth = [len(item["orders"][0]) for item in items]
        for step in range(max(depth)):
            for i, item in enumerate(items):
                for part in range(item["parts"]):
                    if step < depth[i]:
                        send(i, part, step, 0, part_of(ins[i], item, part, None), coords)
        for i, item in enumerate(items):
            for part in range(item["parts"]):
                own = part_of(outs[i], item, part, item["cube"].flat(coords))
                one = pltpu.make_async_copy(
                    part_of(ins[i], item, part, None), own, sems[3 * i + 2].at[part]
                )
                one.start()
                pending.append(one.wait)
        for step in range(max(depth)):
            for k in range(1 << step):
                for i, item in enumerate(items):
                    if step >= depth[i]:
                        continue
                    for part in range(item["parts"]):
                        pattern = k + (1 << step)
                        pos = moved(coords, item["orders"][part], pattern)
                        here = part_of(outs[i], item, part, item["cube"].flat(pos))
                        copy(i, part, step, pattern - 1, here, here).wait_recv()
                        for later in range(step + 1, depth[i]):
                            send(i, part, later, pattern, here, pos)
        for wait in pending:
            wait()

    shapes, scratch = [], []
    for item in items:
        n = item["cube"].total
        whole = (item["rows"], item["cols"] * n) if item["lanes"] else (item["rows"] * n, item["cols"])
        shapes.append(jax.ShapeDtypeStruct(whole, item["dtype"]))
        scratch += [pltpu.SemaphoreType.DMA((item["parts"], n - 1))] * 2
        scratch.append(pltpu.SemaphoreType.DMA((item["parts"],)))
    moved_bytes = sum(s.size * s.dtype.itemsize for s in shapes)
    return pl.pallas_call(
        kernel,
        out_shape=shapes,
        in_specs=[pl.BlockSpec(memory_space=pltpu.VMEM)] * count,
        out_specs=[pl.BlockSpec(memory_space=pl.ANY)] * count,
        scratch_shapes=scratch,
        compiler_params=pltpu.CompilerParams(collective_id=collective_id, has_side_effects=True),
        cost_estimate=pl.CostEstimate(flops=0, bytes_accessed=8 * moved_bytes, transcendentals=0),
        name="cube_gather",
    )(*[block[0] for block in blocks])


def cube_reduce(blocks, collective_id):
    items = []
    for array, axes, lanes, parts in blocks:
        cube = Cube(axes)
        rows, cols = array.shape
        rows, cols = (rows, cols // cube.total) if lanes else (rows // cube.total, cols)
        orders = [order[::-1] for order in gather_orders(axes)]
        items.append(
            dict(rows=rows, cols=cols, lanes=lanes, parts=parts, cube=cube, orders=orders, dtype=array.dtype)
        )
    count = len(items)
    names = [a for a in BOTH if any(a in item["cube"].axes for item in items)]

    def kernel(*refs):
        ins, outs = refs[:count], refs[count : 2 * count]
        scratch = refs[2 * count :]
        coords = {a: lax.axis_index(a) for a in names}
        held = [scratch[5 * i] for i in range(count)]
        came = [scratch[5 * i + 1] for i in range(count)]
        send_sem = [scratch[5 * i + 2] for i in range(count)]
        recv_sem = [scratch[5 * i + 3] for i in range(count)]
        load_sem = [scratch[5 * i + 4] for i in range(count)]
        depth = [len(item["orders"][0]) for item in items]
        pending = []

        def load(i, part, k):
            item = items[i]
            pos = moved(coords, item["orders"][part], k << 1)
            return pltpu.make_async_copy(
                part_of(ins[i], item, part, item["cube"].flat(pos)),
                held[i].at[part, k],
                load_sem[i].at[part, k],
            )

        for i, item in enumerate(items):
            for part in range(item["parts"]):
                for k in range(1 << (depth[i] - 1)):
                    load(i, part, k).start()
        greet(coords, [order for item in items for order in item["orders"]])

        def base(i, step):
            return (1 << depth[i]) - (1 << (depth[i] - step))

        def copy(i, part, step, k, src):
            name, bit = items[i]["orders"][part][step]
            slot = base(i, step) + k
            return pltpu.make_async_remote_copy(
                src_ref=src,
                dst_ref=came[i].at[part, slot],
                send_sem=send_sem[i].at[part, slot],
                recv_sem=recv_sem[i].at[part, slot],
                device_id={name: flipped(coords, name, bit)[name]},
                device_id_type=pl.DeviceIdType.MESH,
            )

        def first(count_bits):
            return sorted(range(1 << count_bits), key=lambda k: -(k & 1))

        for i, item in enumerate(items):
            for k in first(depth[i] - 1):
                for part in range(item["parts"]):
                    pos = moved(coords, item["orders"][part], (k << 1) | 1)
                    one = copy(i, part, 0, k, part_of(ins[i], item, part, item["cube"].flat(pos)))
                    one.start()
                    pending.append(one.wait_send)

        def add_up(i, part, pattern, steps, store):
            item = items[i]
            rows = item["rows"] // item["parts"]
            load(i, part, pattern >> 1).wait()
            for step in range(steps):
                k = pattern >> (step + 1)
                copy(i, part, step, k, came[i].at[part, base(i, step) + k]).wait_recv()
            chunk = 16 if rows % 16 == 0 else 8

            def one_chunk(c, carry):
                where = pl.ds(pl.multiple_of(c * chunk, chunk), chunk)
                total = held[i][part, pattern >> 1, where, :].astype(jnp.float32)
                for step in range(steps):
                    slot = base(i, step) + (pattern >> (step + 1))
                    total = total + came[i][part, slot, where, :].astype(jnp.float32)
                store(where, total)
                return carry

            lax.fori_loop(0, rows // chunk, one_chunk, 0)

        for step in range(1, max(depth)):
            for i, item in enumerate(items):
                if step >= depth[i]:
                    continue
                for k in first(depth[i] - step - 1):
                    for part in range(item["parts"]):
                        pattern = ((k << 1) | 1) << step

                        def keep(where, total, i=i, part=part, pattern=pattern):
                            held[i][part, pattern >> 1, where, :] = total.astype(held[i].dtype)

                        add_up(i, part, pattern, step, keep)
                        one = copy(i, part, step, k, held[i].at[part, pattern >> 1])
                        one.start()
                        pending.append(one.wait_send)
        for i, item in enumerate(items):
            rows = item["rows"] // item["parts"]
            for part in range(item["parts"]):

                def put(where, total, i=i, part=part, rows=rows):
                    whole = pl.ds(pl.multiple_of(part * rows + where.start, 8), where.size)
                    outs[i][whole, :] = total

                add_up(i, part, 0, depth[i], put)
        for wait in pending:
            wait()

    shapes, scratch = [], []
    for item in items:
        n = item["cube"].total
        block = (item["rows"] // item["parts"], item["cols"])
        shapes.append(jax.ShapeDtypeStruct((item["rows"], item["cols"]), jnp.float32))
        scratch.append(pltpu.VMEM((item["parts"], n // 2) + block, item["dtype"]))
        scratch.append(pltpu.VMEM((item["parts"], n - 1) + block, item["dtype"]))
        scratch += [pltpu.SemaphoreType.DMA((item["parts"], n - 1))] * 2
        scratch.append(pltpu.SemaphoreType.DMA((item["parts"], n // 2)))
    moved_bytes = sum(block[0].size * block[0].dtype.itemsize for block in blocks)
    return pl.pallas_call(
        kernel,
        out_shape=shapes,
        in_specs=[pl.BlockSpec(memory_space=pl.ANY)] * count,
        out_specs=[pl.BlockSpec(memory_space=pltpu.VMEM)] * count,
        scratch_shapes=scratch,
        compiler_params=pltpu.CompilerParams(
            collective_id=collective_id, has_side_effects=True, vmem_limit_bytes=60 << 20
        ),
        cost_estimate=pl.CostEstimate(flops=0, bytes_accessed=8 * moved_bytes, transcendentals=0),
        name="cube_reduce",
    )(*[block[0] for block in blocks])


def rows_dot(left, right):
    return lax.dot_general(left, right, (((1,), (1,)), ((), ())), preferred_element_type=jnp.float32)


def columns_dot(left, right):
    return lax.dot_general(left, right, (((0,), (0,)), ((), ())), preferred_element_type=jnp.float32)


def tile_groups(groups, slots):
    tile = groups
    while tile % 2 == 0 and tile * slots > 1024:
        tile //= 2
    return tile


def expert_calls(rows):
    groups, experts, slots, width = rows.shape
    tile = tile_groups(groups, slots)
    height = tile * slots
    grid = (experts, groups // tile)
    token_spec = pl.BlockSpec((tile, None, slots, width), lambda e, m: (m, e, 0, 0))
    params = pltpu.CompilerParams(
        dimension_semantics=("arbitrary", "arbitrary"), vmem_limit_bytes=60 << 20
    )
    return groups, experts, slots, width, height, grid, token_spec, params


def expert_first(rows, cots, gate, weight_in, weight_out):
    groups, experts, slots, width, height, grid, token_spec, params = expert_calls(rows)
    units = weight_out.shape[1]

    def kernel(rows_ref, cots_ref, gate_ref, in_ref, out_ref, back_ref, act_ref, pre_ref, grad_ref):
        picked = rows_ref[...].reshape(height, width)
        gate_pre = rows_dot(picked, in_ref[0])
        up_pre = rows_dot(picked, in_ref[1])
        raw = rows_dot(cots_ref[...].reshape(height, width), out_ref[...])
        weight = gate_ref[...]
        sigm = jax.nn.sigmoid(gate_pre)
        silu = gate_pre * sigm
        act = silu * up_pre
        grad_ref[...] = jnp.sum(act * raw, axis=1, keepdims=True)
        act_ref[...] = (act * weight).astype(jnp.bfloat16)
        hidden_grad = raw * weight
        gate_part = (hidden_grad * up_pre * sigm * (1.0 + gate_pre * (1.0 - sigm))).astype(
            jnp.bfloat16
        )
        up_part = (hidden_grad * silu).astype(jnp.bfloat16)
        pre_ref[0] = gate_part
        pre_ref[1] = up_part
        back = jnp.dot(gate_part, in_ref[0], preferred_element_type=jnp.float32)
        back = back + jnp.dot(up_part, in_ref[1], preferred_element_type=jnp.float32)
        back_ref[...] = back.astype(jnp.bfloat16).reshape(back_ref.shape)

    count = groups * slots
    column = pl.BlockSpec((None, height, 1), lambda e, m: (e, m, 0))
    work = experts * count * width * units
    return pl.pallas_call(
        kernel,
        grid=grid,
        out_shape=[
            jax.ShapeDtypeStruct(rows.shape, jnp.bfloat16),
            jax.ShapeDtypeStruct((experts, count, units), jnp.bfloat16),
            jax.ShapeDtypeStruct((experts, 2, count, units), jnp.bfloat16),
            jax.ShapeDtypeStruct((experts, count, 1), jnp.float32),
        ],
        in_specs=[
            token_spec,
            token_spec,
            column,
            pl.BlockSpec((None, 2, units, width), lambda e, m: (e, 0, 0, 0)),
            pl.BlockSpec((None, units, width), lambda e, m: (e, 0, 0)),
        ],
        out_specs=[
            token_spec,
            pl.BlockSpec((None, height, units), lambda e, m: (e, m, 0)),
            pl.BlockSpec((None, 2, height, units), lambda e, m: (e, 0, m, 0)),
            column,
        ],
        compiler_params=params,
        cost_estimate=pl.CostEstimate(
            flops=10 * work, bytes_accessed=6 * rows.size + 6 * experts * units * width, transcendentals=0
        ),
        name="expert_first",
    )(rows, cots, gate, weight_in, weight_out)


def expert_second(rows, cots, act, pre_grad, weight_out):
    groups, experts, slots, width, height, grid, token_spec, params = expert_calls(rows)
    units = weight_out.shape[1]

    def kernel(rows_ref, cots_ref, act_ref, pre_ref, out_ref, rows_out_ref, in_grad_ref, out_grad_ref):
        act_low = act_ref[...]
        result = jnp.dot(act_low, out_ref[...], preferred_element_type=jnp.float32)
        rows_out_ref[...] = result.astype(jnp.bfloat16).reshape(rows_out_ref.shape)
        picked = rows_ref[...].reshape(height, width)
        out_part = columns_dot(act_low, cots_ref[...].reshape(height, width))
        gate_part = columns_dot(pre_ref[0], picked)
        up_part = columns_dot(pre_ref[1], picked)

        @pl.when(pl.program_id(1) == 0)
        def _():
            out_grad_ref[...] = out_part
            in_grad_ref[0] = gate_part
            in_grad_ref[1] = up_part

        @pl.when(pl.program_id(1) != 0)
        def _():
            out_grad_ref[...] += out_part
            in_grad_ref[0] += gate_part
            in_grad_ref[1] += up_part

    count = groups * slots
    work = experts * count * width * units
    return pl.pallas_call(
        kernel,
        grid=grid,
        out_shape=[
            jax.ShapeDtypeStruct(rows.shape, jnp.bfloat16),
            jax.ShapeDtypeStruct((experts, 2, units, width), jnp.float32),
            jax.ShapeDtypeStruct((experts, units, width), jnp.float32),
        ],
        in_specs=[
            token_spec,
            token_spec,
            pl.BlockSpec((None, height, units), lambda e, m: (e, m, 0)),
            pl.BlockSpec((None, 2, height, units), lambda e, m: (e, 0, m, 0)),
            pl.BlockSpec((None, units, width), lambda e, m: (e, 0, 0)),
        ],
        out_specs=[
            token_spec,
            pl.BlockSpec((None, 2, units, width), lambda e, m: (e, 0, 0, 0)),
            pl.BlockSpec((None, units, width), lambda e, m: (e, 0, 0)),
        ],
        compiler_params=params,
        cost_estimate=pl.CostEstimate(
            flops=8 * work, bytes_accessed=6 * rows.size + 14 * experts * units * width, transcendentals=0
        ),
        name="expert_second",
    )(rows, cots, act, pre_grad, weight_out)


def halves(rows):
    return 2 if rows % 32 == 0 else 1


def body(
    tokens,
    segments,
    routes,
    cotangent,
    attention_gain,
    latent_gain,
    feedforward_gain,
    query_weight,
    latent_weight,
    expand_weight,
    output_weight,
    router_weight,
    shared_in,
    shared_out,
    expert_in,
    expert_out,
):
    own_rows, width = tokens.shape
    groups = lax.axis_size("dp")
    place_dp = lax.axis_index("dp")
    first_row = lax.axis_index("tensor") * own_rows
    local_experts = expert_in.shape[0]
    segment_row = segments[0]
    gain_rows, lat_rows = attention_gain.shape[0], latent_gain.shape[0]
    columns = jnp.stack(
        [attention_gain, feedforward_gain, jnp.pad(latent_gain, (0, gain_rows - lat_rows))], axis=1
    )
    router_block = jnp.concatenate([router_weight, columns], axis=1)
    router_block = jnp.pad(router_block, ((0, 0), (0, -router_block.shape[1] % 128)))
    routes_block = jnp.pad(routes.T, ((0, -routes.shape[1] % 8), (0, 0)), constant_values=-1)
    (
        group_rows,
        cot_group,
        latent_full,
        query_full,
        expand_full,
        router_block_full,
        routes_full,
        output_full,
    ) = gather_blocks(
        [
            (tokens, ("tensor",), False, halves(own_rows)),
            (cotangent, ("tensor",), False, halves(own_rows)),
            (latent_weight, BOTH, False, halves(latent_weight.shape[0])),
            (query_weight, ("dp",), False, halves(query_weight.shape[0])),
            (expand_weight, ("dp",), False, halves(expand_weight.shape[0])),
            (router_block, BOTH, False, halves(router_block.shape[0])),
            (routes_block, ("dp",), True, 1),
            (output_weight, ("dp",), True, halves(output_weight.shape[0])),
        ],
        0,
    )
    row_count = group_rows.shape[0]
    router_full = router_block_full[:, :EXPERTS]
    gain_one = router_block_full[:, EXPERTS].astype(jnp.float32)
    gain_two = router_block_full[:, EXPERTS + 1].astype(jnp.float32)
    gain_lat_low = router_block_full[:, EXPERTS + 2].reshape(-1, gain_rows)[:, :lat_rows].reshape(-1)
    routes_all = routes_full[: routes.shape[1]]
    cot_all = gather(cot_group, "dp").reshape(groups, row_count, width)

    wide = group_rows.astype(jnp.float32)
    scale_one = rms_scale(wide)
    normed = (wide * scale_one * gain_one).astype(jnp.bfloat16)
    cosine, sine = rope_tables(segment_row)
    query, key_rows, value_rows, compressed, latent_scale, latent_normed = attention_tables(
        normed, query_full, latent_full, expand_full, gain_lat_low, cosine, sine
    )
    mixed, logsum = attend(query, key_rows, value_rows, segment_row)
    mixed_flat = mixed.reshape(row_count, -1)
    attention_part = jnp.dot(mixed_flat, output_full, preferred_element_type=jnp.float32)
    (attention_own,) = reduce_blocks(
        [(attention_part.astype(jnp.bfloat16), ("tensor",), False, halves(own_rows))], 1
    )
    wide_own = tokens.astype(jnp.float32)
    hidden = wide_own + attention_own
    scale_two = rms_scale(hidden)
    normed_two_own = (hidden * scale_two * gain_two).astype(jnp.bfloat16)

    (normed_flat,) = gather_blocks([(normed_two_own, BOTH, False, halves(own_rows))], 2)
    normed_flat, shared_in, shared_out, cot_all = lax.optimization_barrier(
        (normed_flat, shared_in, shared_out, cot_all)
    )
    shared_in_full = gather(shared_in, "dp")
    shared_out_full = gather(shared_out, "dp", 1)
    normed_all = normed_flat.reshape(groups, row_count, width)
    normed_two = lax.dynamic_index_in_dim(normed_all, place_dp, 0, keepdims=False)

    expert_ids = jnp.arange(EXPERTS, dtype=jnp.int32)
    chosen = jnp.any(routes_all[:, :, None] == expert_ids[None, None, :], axis=0)
    logits = jnp.dot(normed_flat, router_full, preferred_element_type=jnp.float32)
    sigm = jnp.where(chosen, jax.nn.sigmoid(logits), 0.0)
    picked_total = jnp.sum(sigm, axis=1, keepdims=True)
    gate_dense = route_scale * sigm / picked_total
    first_expert = place_dp * local_experts
    gate_local = lax.dynamic_slice_in_dim(gate_dense, first_expert, local_experts, 1)
    chosen_local = lax.dynamic_slice_in_dim(
        chosen.astype(jnp.bfloat16), first_expert, local_experts, 1
    ).reshape(groups, row_count, local_experts)
    gate_local = jnp.swapaxes(gate_local.reshape(groups, row_count, local_experts), 1, 2)
    places = jnp.arange(row_count, dtype=jnp.int32)
    below = (places[None, :] < places[:, None]).astype(jnp.bfloat16)
    rank = jnp.einsum("ts,gse->get", below, chosen_local, preferred_element_type=jnp.float32)
    slot = jnp.where(jnp.swapaxes(chosen_local, 1, 2) > 0, rank, -1.0).astype(jnp.int32)
    slots = CAP + -CAP % 16
    is_slot = slot[:, :, None, :] == jnp.arange(slots, dtype=jnp.int32)[None, None, :, None]
    pick = is_slot.astype(jnp.bfloat16).reshape(groups, local_experts * slots, row_count)
    gate_slot = jnp.sum(jnp.where(is_slot, gate_local[:, :, None, :], 0.0), axis=-1)

    rows = jnp.einsum(
        "gst,gtd->gsd", pick, normed_all, preferred_element_type=jnp.float32
    ).astype(jnp.bfloat16).reshape(groups, local_experts, slots, width)
    cots = jnp.einsum(
        "gst,gtd->gsd", pick, cot_all, preferred_element_type=jnp.float32
    ).astype(jnp.bfloat16).reshape(groups, local_experts, slots, width)
    gate_column = jnp.swapaxes(gate_slot, 0, 1).reshape(local_experts, groups * slots, 1)
    back_slots, act_gated, expert_pre_grad, gate_grad_column = expert_first(
        rows, cots, gate_column, jnp.transpose(expert_in, (0, 2, 3, 1)), expert_out
    )
    out_slots, expert_in_grad, expert_out_grad = expert_second(
        rows, cots, act_gated, expert_pre_grad, expert_out
    )
    back_slots = back_slots.reshape(groups, local_experts * slots, width)
    out_slots = out_slots.reshape(groups, local_experts * slots, width)
    expert_in_grad = jnp.transpose(expert_in_grad, (0, 3, 1, 2))
    gate_grad_slot = jnp.swapaxes(gate_grad_column.reshape(local_experts, groups, slots), 0, 1)
    gate_grad_local = jnp.sum(jnp.where(is_slot, gate_grad_slot[..., None], 0.0), axis=2)
    gate_grad_all = lax.dynamic_update_slice_in_dim(
        jnp.zeros((groups * row_count, 2 * EXPERTS), jnp.bfloat16),
        jnp.swapaxes(gate_grad_local, 1, 2)
        .reshape(groups * row_count, local_experts)
        .astype(jnp.bfloat16),
        first_expert,
        1,
    )

    shared_pre = jnp.einsum(
        "gd,dcf->gcf", normed_two, shared_in_full, preferred_element_type=jnp.float32
    )
    shared_act = (jax.nn.silu(shared_pre[:, 0]) * shared_pre[:, 1]).astype(jnp.bfloat16)
    shared_part = jnp.dot(shared_act, shared_out_full, preferred_element_type=jnp.float32)
    shared_hidden_grad = jnp.dot(cot_group, shared_out_full.T, preferred_element_type=jnp.float32)
    shared_gate_part, shared_up_part = swiglu_grad(
        shared_hidden_grad, shared_pre[:, 0], shared_pre[:, 1]
    )
    shared_pre_grad = jnp.stack([shared_gate_part, shared_up_part], axis=1).astype(jnp.bfloat16)
    shared_out_grad = jnp.dot(
        shared_act.T, cot_group, preferred_element_type=jnp.float32
    ).astype(jnp.bfloat16)
    shared_in_grad = jnp.einsum(
        "gcf,gd->cfd", shared_pre_grad, normed_two, preferred_element_type=jnp.float32
    ).astype(jnp.bfloat16)
    shared_back = jnp.einsum(
        "gcf,dcf->gd", shared_pre_grad, shared_in_full, preferred_element_type=jnp.float32
    )

    def combine(slot_rows):
        total = jnp.einsum("gst,gsd->gtd", pick, slot_rows, preferred_element_type=jnp.float32)
        return total.astype(jnp.bfloat16).reshape(groups * row_count, width)

    back_group = scatter_sum(combine(back_slots), "dp")
    out_sum = combine(out_slots)
    (
        back_group,
        out_sum,
        expert_out_grad,
        expert_in_grad,
        shared_out_grad,
        shared_in_grad,
        shared_back,
        shared_part,
        gate_grad_all,
    ) = lax.optimization_barrier(
        (
            back_group,
            out_sum,
            expert_out_grad,
            expert_in_grad,
            shared_out_grad,
            shared_in_grad,
            shared_back,
            shared_part,
            gate_grad_all,
        )
    )
    gate_grad_own, back_own = reduce_blocks(
        [
            (gate_grad_all, BOTH, False, 1),
            (
                (back_group.astype(jnp.float32) + shared_back).astype(jnp.bfloat16),
                ("tensor",),
                False,
                halves(own_rows),
            ),
        ],
        3,
    )
    out_group = scatter_sum(out_sum, "dp")

    first_token = place_dp * row_count + first_row
    sigm_own = own_slice(sigm, first_token, own_rows)
    total_own = own_slice(picked_total, first_token, own_rows)
    gate_grad = gate_grad_own[:, :EXPERTS]
    picked_grad = route_scale * (
        gate_grad / total_own
        - jnp.sum(gate_grad * sigm_own, axis=1, keepdims=True) / (total_own * total_own)
    )
    logit_grad = picked_grad * sigm_own * (1.0 - sigm_own)
    router_grad = jnp.dot(
        normed_two_own.astype(jnp.float32).T, logit_grad, precision=lax.Precision.HIGHEST
    )
    router_back = jnp.dot(
        logit_grad, router_full.astype(jnp.float32).T, precision=lax.Precision.HIGHEST
    )
    normed_two_grad = back_own + router_back
    weighted_two = normed_two_grad * gain_two
    hidden_grad = (
        cotangent.astype(jnp.float32)
        + scale_two * weighted_two
        - hidden * scale_two**3 * jnp.mean(hidden * weighted_two, axis=-1, keepdims=True)
    )
    gain_two_grad = jnp.sum(normed_two_grad * hidden * scale_two, axis=0)
    (hidden_low,) = gather_blocks(
        [(hidden_grad.astype(jnp.bfloat16), ("tensor",), False, halves(own_rows))], 4
    )

    hidden_units = shared_in.shape[2]
    output_grad = jnp.dot(mixed_flat.T, hidden_low, preferred_element_type=jnp.float32)
    mixed_grad = (
        jnp.dot(hidden_low, output_full.T, preferred_element_type=jnp.float32)
        .astype(jnp.bfloat16)
        .reshape(mixed.shape)
    )
    query_grad, key_grad, value_grad = attend_back(
        query, key_rows, value_rows, segment_row, mixed_grad, logsum
    )
    query_pre = (
        jnp.concatenate(
            [
                query_grad[..., :DN],
                unrotate(query_grad[..., DN:], cosine[:, None, :], sine[:, None, :]),
            ],
            axis=-1,
        )
        .astype(jnp.bfloat16)
        .reshape(row_count, -1)
    )
    query_pre, out_group = lax.optimization_barrier((query_pre, out_group))
    out_group = (out_group.astype(jnp.float32) + shared_part).astype(jnp.bfloat16)
    out_own = scatter_sum(out_group, "tensor").astype(jnp.float32)
    query_grad_weight = jnp.dot(normed.T, query_pre, preferred_element_type=jnp.float32)
    normed_grad = jnp.dot(query_pre, query_full.T, preferred_element_type=jnp.float32)
    keyvalue_grad = (
        jnp.concatenate([key_grad[..., :DN], value_grad], axis=-1)
        .astype(jnp.bfloat16)
        .reshape(row_count, -1)
    )
    expand_grad = jnp.dot(latent_normed.T, keyvalue_grad, preferred_element_type=jnp.float32)
    latent_normed_grad = jnp.dot(keyvalue_grad, expand_full.T, preferred_element_type=jnp.float32)
    rope_grad = unrotate(jnp.sum(key_grad[..., DN:], axis=1), cosine, sine)
    lat_weighted = latent_normed_grad * gain_lat_low.astype(jnp.float32)
    gain_lat_grad = jnp.sum(latent_normed_grad * compressed * latent_scale, axis=0)
    compressed_grad = latent_scale * lat_weighted - compressed * latent_scale**3 * jnp.mean(
        compressed * lat_weighted, axis=-1, keepdims=True
    )
    latent_grad = jnp.concatenate([compressed_grad, rope_grad], axis=-1).astype(jnp.bfloat16)
    latent_grad_weight = jnp.dot(normed.T, latent_grad, preferred_element_type=jnp.float32)
    normed_grad = normed_grad + jnp.dot(
        latent_grad, latent_full.T, preferred_element_type=jnp.float32
    )
    gain_one_grad = jnp.sum(normed_grad * wide * scale_one, axis=0)

    total = groups * lax.axis_size("tensor")
    gains = jnp.stack(
        [
            jnp.pad(g.reshape(total, -1), ((0, 0), (0, -(g.shape[0] // total) % 128))).reshape(-1)
            for g in (gain_one_grad, gain_two_grad, gain_lat_grad)
        ]
    )
    gains = jnp.pad(gains, ((0, -gains.shape[0] % 8), (0, 0)))
    hidden_units = shared_in.shape[2]
    (
        latent_out,
        router_out,
        gains_out,
        query_out,
        output_out,
        expand_out,
        shared_in_out,
        shared_out_out,
        normed_own,
    ) = reduce_blocks(
        [
            (latent_grad_weight.astype(jnp.bfloat16), BOTH, False, 1),
            (router_grad.astype(jnp.bfloat16), BOTH, False, 1),
            (gains, BOTH, True, 1),
            (query_grad_weight.astype(jnp.bfloat16), ("dp",), False, halves(query_weight.shape[0])),
            (output_grad.astype(jnp.bfloat16), ("dp",), True, halves(output_weight.shape[0])),
            (expand_grad.astype(jnp.bfloat16), ("dp",), False, halves(expand_weight.shape[0])),
            (
                shared_in_grad.reshape(2 * hidden_units, width),
                ("dp",),
                True,
                halves(2 * hidden_units),
            ),
            (shared_out_grad, ("dp",), True, halves(hidden_units)),
            (normed_grad.astype(jnp.bfloat16), ("tensor",), False, halves(own_rows)),
        ],
        5,
    )
    shared_in_out = jnp.moveaxis(shared_in_out.reshape(2, hidden_units, -1), 2, 0)
    gain_one_out = gains_out[0, :gain_rows]
    gain_two_out = gains_out[1, :gain_rows]
    gain_lat_out = gains_out[2, :lat_rows]
    scale_own = own_slice(scale_one, first_row, own_rows)
    weighted_one = normed_own * gain_one
    tokens_grad = (
        hidden_grad
        + scale_own * weighted_one
        - wide_own * scale_own**3 * jnp.mean(wide_own * weighted_one, axis=-1, keepdims=True)
    )
    out_tokens = (hidden + out_own).astype(jnp.bfloat16)
    return (
        out_tokens,
        tokens_grad,
        gain_one_out,
        gain_lat_out,
        gain_two_out,
        query_out,
        latent_out,
        expand_out,
        output_out,
        router_out,
        shared_in_out,
        shared_out_out,
        expert_in_grad,
        expert_out_grad,
    )


def solution(mesh):
    placed = (
        P(("dp", "tensor"), None),
        P("dp", None),
        P("dp", None),
        P(("dp", "tensor"), None),
        P(("dp", "tensor")),
        P(("dp", "tensor")),
        P(("dp", "tensor")),
        P("dp", "tensor"),
        P(("dp", "tensor"), None),
        P("dp", "tensor"),
        P("tensor", "dp"),
        P(("dp", "tensor"), None),
        P("dp", None, "tensor"),
        P("tensor", "dp"),
        P("dp", None, None, "tensor"),
        P("dp", "tensor", None),
    )
    return jax.shard_map(
        body,
        mesh=mesh,
        in_specs=placed,
        out_specs=(
            P(("dp", "tensor"), None),
            P(("dp", "tensor"), None),
            P(("dp", "tensor")),
            P(("dp", "tensor")),
            P(("dp", "tensor")),
            P("dp", "tensor"),
            P(("dp", "tensor"), None),
            P("dp", "tensor"),
            P("tensor", "dp"),
            P(("dp", "tensor"), None),
            P("dp", None, "tensor"),
            P("tensor", "dp"),
            P("dp", None, None, "tensor"),
            P("dp", "tensor", None),
        ),
        check_vma=False,
    )
```
